32 devices in a mesh: dp: 4 (over y, z), cp: 8 (over x, core).
Axes of the slice: x: 4, y: 2, z: 2, core: 2. Of those that a mesh axis runs over, the one named last changes fastest.
The devices are a block of a 4x4x8 slice.
Arguments:
- q_raw: bfloat16 [16384, 32, 128], P(('dp', 'cp')), parts along dimension 0
- k_raw: bfloat16 [16384, 8, 128], P(('dp', 'cp')), parts along dimension 0
- v_proj: bfloat16 [16384, 8, 128], P(('dp', 'cp')), parts along dimension 0
- out_fwd: bfloat16 [16384, 32, 128], P(('dp', 'cp')), parts along dimension 0
- lse_fwd: float32 [16384, 32], P(('dp', 'cp')), parts along dimension 0
- d_out: bfloat16 [16384, 32, 128], P(('dp', 'cp')), parts along dimension 0
- q_norm: float32 [128], replicated
- k_norm: float32 [128], replicated
Outputs:
- output 1: bfloat16 [16384, 32, 128], P(('dp', 'cp')), parts along dimension 0
- output 2: bfloat16 [16384, 8, 128], P(('dp', 'cp')), parts along dimension 0
- output 3: bfloat16 [16384, 8, 128], P(('dp', 'cp')), parts along dimension 0
- output 4: float32 [512], P('dp'), parts along dimension 0
- output 5: float32 [512], P('dp'), parts along dimension 0
There are 4 independent parts. The reference program is written for one: setup_inputs(seed, part) draws one part's arguments, and reference() takes and returns one part's arrays. A program takes and returns all parts, laid end to end along the dimension named above; an argument that names none is the same for every part.
All inputs are finite; a program needn't handle non-finite values.
Results may differ from the reference program's by a relative error of at most 0.00271093.
Values are sent between devices in bfloat16 or wider.
A program may use at most 768 MiB of HBM per device.

```python
import jax
import jax.numpy as jnp
from jax import lax

HEADS = 32
KV_HEADS = 8
HEAD_DIM = 128
CHUNK = 256
CP_RANKS = 8
QUERY_BLOCK = 64
SEQ_LEN = 2 * CP_RANKS * CHUNK
Q_PER_KV = HEADS // KV_HEADS
BLOCK_COUNT = SEQ_LEN // QUERY_BLOCK
ROPE_THETA = 1000000.0
NORM_EPS = 1e-6


def layout_positions():
    row_ids = jnp.arange(SEQ_LEN)
    owner_dev = row_ids // (2 * CHUNK)
    within = row_ids % (2 * CHUNK)
    chunk_id = jnp.where(within < CHUNK, owner_dev, 2 * CP_RANKS - 1 - owner_dev)
    return chunk_id * CHUNK + within % CHUNK


def rope_tables(positions):
    inv_freq = ROPE_THETA ** (-jnp.arange(0, HEAD_DIM, 2).astype(jnp.float32) / HEAD_DIM)
    angles = positions.astype(jnp.float32)[:, None] * inv_freq[None, :]
    angles = jnp.concatenate([angles, angles], axis=-1)
    return jnp.cos(angles)[:, None, :], jnp.sin(angles)[:, None, :]


def norm_rope(raw_in, weight, cos_t, sin_t):
    mean_sq = jnp.mean(raw_in * raw_in, axis=-1, keepdims=True)
    normed = raw_in * lax.rsqrt(mean_sq + NORM_EPS) * weight
    half_dim = raw_in.shape[-1] // 2
    rotated = jnp.concatenate([-normed[..., half_dim:], normed[..., :half_dim]], axis=-1)
    return normed * cos_t + rotated * sin_t


def forward_stats(q_raw, k_raw, v_proj, q_norm, k_norm):
    positions = layout_positions()
    cos_t, sin_t = rope_tables(positions)
    q_b = norm_rope(q_raw.astype(jnp.float32), q_norm, cos_t, sin_t).astype(jnp.bfloat16)
    k_b = norm_rope(k_raw.astype(jnp.float32), k_norm, cos_t, sin_t).astype(jnp.bfloat16)
    q_f = q_b.astype(jnp.float32).reshape(BLOCK_COUNT, QUERY_BLOCK, KV_HEADS, Q_PER_KV, HEAD_DIM)
    k_f = k_b.astype(jnp.float32)
    v_f = v_proj.astype(jnp.float32)
    sm_scale = HEAD_DIM ** -0.5

    def one_block(scan_in):
        q_blk, q_pos = scan_in
        logits = jnp.einsum('qngd,knd->qngk', q_blk, k_f) * sm_scale
        visible = (q_pos[:, None] >= positions[None, :])[:, None, None, :]
        logits = jnp.where(visible, logits, -jnp.inf)
        row_max = jnp.max(logits, axis=-1, keepdims=True)
        weights = jnp.exp(logits - row_max)
        row_sum = jnp.sum(weights, axis=-1, keepdims=True)
        out_blk = jnp.einsum('qngk,knd->qngd', weights / row_sum, v_f)
        lse_blk = (row_max + jnp.log(row_sum))[..., 0]
        return out_blk, lse_blk

    out_blocks, lse_blocks = lax.map(one_block, (q_f, positions.reshape(BLOCK_COUNT, QUERY_BLOCK)))
    out_fwd = out_blocks.reshape(SEQ_LEN, HEADS, HEAD_DIM).astype(jnp.bfloat16)
    return out_fwd, lse_blocks.reshape(SEQ_LEN, HEADS)


def setup_inputs(seed: int = 0, part: int = 0) -> dict:
    base_key = jax.random.key(seed)
    shared_key, part_key = jax.random.split(base_key)
    part_key = jax.random.fold_in(part_key, part)
    part_keys = jax.random.split(part_key, 4)
    shared_keys = jax.random.split(shared_key, 2)
    q_raw = jax.random.normal(part_keys[0], (SEQ_LEN, HEADS, HEAD_DIM), jnp.float32).astype(jnp.bfloat16)
    k_raw = jax.random.normal(part_keys[1], (SEQ_LEN, KV_HEADS, HEAD_DIM), jnp.float32).astype(jnp.bfloat16)
    v_proj = jax.random.normal(part_keys[2], (SEQ_LEN, KV_HEADS, HEAD_DIM), jnp.float32).astype(jnp.bfloat16)
    d_out = jax.random.normal(part_keys[3], (SEQ_LEN, HEADS, HEAD_DIM), jnp.float32).astype(jnp.bfloat16)
    q_norm = jax.random.uniform(shared_keys[0], (HEAD_DIM,), jnp.float32, minval=0.5, maxval=1.6)
    k_norm = jax.random.uniform(shared_keys[1], (HEAD_DIM,), jnp.float32, minval=0.5, maxval=1.6)
    out_fwd, lse_fwd = forward_stats(q_raw, k_raw, v_proj, q_norm, k_norm)
    return {'q_raw': q_raw, 'k_raw': k_raw, 'v_proj': v_proj, 'out_fwd': out_fwd, 'lse_fwd': lse_fwd, 'd_out': d_out, 'q_norm': q_norm, 'k_norm': k_norm}


def reference(q_raw, k_raw, v_proj, out_fwd, lse_fwd, d_out, q_norm, k_norm):
    positions = layout_positions()
    cos_t, sin_t = rope_tables(positions)
    q_full, pull_q = jax.vjp(lambda raw_in, weight: norm_rope(raw_in, weight, cos_t, sin_t), q_raw.astype(jnp.float32), q_norm)
    k_full, pull_k = jax.vjp(lambda raw_in, weight: norm_rope(raw_in, weight, cos_t, sin_t), k_raw.astype(jnp.float32), k_norm)
    q_f = q_full.astype(jnp.bfloat16).astype(jnp.float32)
    k_f = k_full.astype(jnp.bfloat16).astype(jnp.float32)
    v_f = v_proj.astype(jnp.float32)
    do_f = d_out.astype(jnp.float32)
    delta_sum = jnp.sum(do_f * out_fwd.astype(jnp.float32), axis=-1)
    sm_scale = HEAD_DIM ** -0.5
    scan_in = (q_f.reshape(BLOCK_COUNT, QUERY_BLOCK, KV_HEADS, Q_PER_KV, HEAD_DIM),
               do_f.reshape(BLOCK_COUNT, QUERY_BLOCK, KV_HEADS, Q_PER_KV, HEAD_DIM),
               lse_fwd.reshape(BLOCK_COUNT, QUERY_BLOCK, KV_HEADS, Q_PER_KV),
               delta_sum.reshape(BLOCK_COUNT, QUERY_BLOCK, KV_HEADS, Q_PER_KV),
               positions.reshape(BLOCK_COUNT, QUERY_BLOCK))

    def scan_step(loop_state, block_in):
        dk_acc, dv_acc = loop_state
        q_blk, do_blk, lse_blk, delta_blk, q_pos = block_in
        logits = jnp.einsum('qngd,knd->qngk', q_blk, k_f) * sm_scale - lse_blk[..., None]
        visible = (q_pos[:, None] >= positions[None, :])[:, None, None, :]
        attn_prob = jnp.exp(jnp.where(visible, logits, -jnp.inf))
        attn_dprob = jnp.einsum('qngd,knd->qngk', do_blk, v_f)
        score_grad = (attn_prob * (attn_dprob - delta_blk[..., None])).astype(jnp.bfloat16).astype(jnp.float32)
        prob_bf = attn_prob.astype(jnp.bfloat16).astype(jnp.float32)
        dq_blk = sm_scale * jnp.einsum('qngk,knd->qngd', score_grad, k_f)
        dk_acc = dk_acc + sm_scale * jnp.einsum('qngk,qngd->knd', score_grad, q_blk)
        dv_acc = dv_acc + jnp.einsum('qngk,qngd->knd', prob_bf, do_blk)
        return (dk_acc, dv_acc), dq_blk

    zero_kv = jnp.zeros((SEQ_LEN, KV_HEADS, HEAD_DIM), jnp.float32)
    (dk_sum, dv_sum), dq_blocks = lax.scan(scan_step, (zero_kv, zero_kv), scan_in)
    dq_raw, dq_norm = pull_q(dq_blocks.reshape(SEQ_LEN, HEADS, HEAD_DIM))
    dk_raw, dk_norm = pull_k(dk_sum)
    return (dq_raw.astype(jnp.bfloat16), dk_raw.astype(jnp.bfloat16), dv_sum.astype(jnp.bfloat16), dq_norm, dk_norm)
```

```python
import functools

import jax
import jax.numpy as jnp
from jax import lax
from jax.experimental import pallas as pl
from jax.experimental.pallas import tpu as pltpu
from jax.sharding import PartitionSpec as P

HEAD_DIM = 128
ROPE_THETA = 1000000.0
NORM_EPS = 1e-6
LOG2E = 1.4426950408889634
SM_SCALE = HEAD_DIM ** -0.5
CORES = 2


def rope_tables(positions):
    inv_freq = ROPE_THETA ** (-jnp.arange(0, HEAD_DIM, 2).astype(jnp.float32) / HEAD_DIM)
    angles = positions.astype(jnp.float32)[..., None] * inv_freq
    angles = jnp.concatenate([angles, angles], axis=-1)
    return jnp.cos(angles), jnp.sin(angles)


def norm_rope(raw_in, weight, cos_t, sin_t):
    mean_sq = jnp.mean(raw_in * raw_in, axis=-1, keepdims=True)
    normed = raw_in * lax.rsqrt(mean_sq + NORM_EPS) * weight
    half_dim = raw_in.shape[-1] // 2
    rotated = jnp.concatenate([-normed[..., half_dim:], normed[..., :half_dim]], axis=-1)
    return normed * cos_t + rotated * sin_t


def dot(a, b, dims):
    return lax.dot_general(a, b, (dims, ((), ())), preferred_element_type=jnp.float32)


def attn_kernel(chunk_len, per_kv, q_ref, do_ref, st_ref, k_ref, v_ref, dq_ref, dk_ref, dv_ref,
                qt_scr, dot_scr, dqt_scr, kt_scr, p_scr, ds_scr):
    chip = lax.axis_index('cp') // CORES
    num_src, num_chunks = k_ref.shape[0], k_ref.shape[2]
    for qb in range(num_chunks):
        qt_scr[qb] = q_ref[0, qb].T
        dot_scr[qb] = do_ref[0, qb].T
    dqt_scr[...] = jnp.zeros_like(dqt_scr)
    dk_ref[...] = jnp.zeros_like(dk_ref)
    dv_ref[...] = jnp.zeros_like(dv_ref)

    def block(src, kc, qb, masked):
        k_blk, v_blk = k_ref[src, 0, kc], v_ref[src, 0, kc]
        if masked:
            key_pos = lax.broadcasted_iota(jnp.int32, (chunk_len, chunk_len), 0)
            query_pos = lax.broadcasted_iota(jnp.int32, (chunk_len, chunk_len), 1)
            visible = key_pos <= query_pos
        for g in range(per_kv):
            cols = pl.ds(g * chunk_len, chunk_len)
            logits = dot(k_blk, qt_scr[qb, :, cols], ((1,), (0,))) * (SM_SCALE * LOG2E) - st_ref[0, qb, 0:1, cols]
            if masked:
                logits = jnp.where(visible, logits, -jnp.inf)
            prob = jnp.exp2(logits)
            dprob = dot(v_blk, dot_scr[qb, :, cols], ((1,), (0,)))
            p_scr[:, cols] = prob.astype(jnp.bfloat16)
            ds_scr[:, cols] = (prob * (dprob - st_ref[0, qb, 1:2, cols])).astype(jnp.bfloat16)
        dv_ref[src, 0, kc] += dot(p_scr[...], do_ref[0, qb], ((1,), (0,)))
        dk_ref[src, 0, kc] += dot(ds_scr[...], q_ref[0, qb], ((1,), (0,)))
        dqt_scr[qb] += dot(kt_scr[...], ds_scr[...], ((1,), (0,)))

    @pl.loop(0, num_src)
    def _(src):
        own = src == chip
        early = src < chip
        num_kc = jnp.where(early, num_chunks // 2, num_chunks)

        @pl.loop(0, num_kc)
        def _(kc):
            kt_scr[...] = k_ref[src, 0, kc].T

            @pl.when(own)
            def _():
                block(src, kc, kc, True)

            first = jnp.where(own, kc + 1, jnp.where(early, 0, num_chunks // 2))

            @pl.loop(first, num_chunks)
            def _(qb):
                block(src, kc, qb, False)

    for qb in range(num_chunks):
        for g in range(per_kv):
            dq_ref[0, qb, g] = dqt_scr[qb, :, g * chunk_len:(g + 1) * chunk_len].T * SM_SCALE


def attn_grads(q, d_out, stats, k_all, v_all):
    kv_heads, num_chunks, rows, _ = q.shape
    num_src, _, _, chunk_len, _ = k_all.shape
    per_kv = rows // chunk_len
    row_spec = pl.BlockSpec((1, num_chunks, rows, HEAD_DIM), lambda h: (h, 0, 0, 0))
    key_spec = pl.BlockSpec((num_src, 1, num_chunks, chunk_len, HEAD_DIM), lambda h: (0, h, 0, 0, 0))
    out_key = jax.ShapeDtypeStruct(k_all.shape, jnp.float32)
    return pl.pallas_call(
        functools.partial(attn_kernel, chunk_len, per_kv),
        grid=(kv_heads,),
        in_specs=[row_spec, row_spec,
                  pl.BlockSpec((1, num_chunks, 2, rows), lambda h: (h, 0, 0, 0)),
                  key_spec, key_spec],
        out_specs=[pl.BlockSpec((1, num_chunks, per_kv, chunk_len, HEAD_DIM), lambda h: (h, 0, 0, 0, 0)), key_spec, key_spec],
        out_shape=[jax.ShapeDtypeStruct((kv_heads, num_chunks, per_kv, chunk_len, HEAD_DIM), jnp.float32), out_key, out_key],
        scratch_shapes=[
            pltpu.VMEM((num_chunks, HEAD_DIM, rows), jnp.bfloat16),
            pltpu.VMEM((num_chunks, HEAD_DIM, rows), jnp.bfloat16),
            pltpu.VMEM((num_chunks, HEAD_DIM, rows), jnp.float32),
            pltpu.VMEM((HEAD_DIM, chunk_len), jnp.bfloat16),
            pltpu.VMEM((chunk_len, rows), jnp.bfloat16),
            pltpu.VMEM((chunk_len, rows), jnp.bfloat16),
        ],
        compiler_params=pltpu.CompilerParams(vmem_limit_bytes=56 * 2 ** 20),
        cost_estimate=pl.CostEstimate(flops=50_000_000_000, bytes_accessed=64_000_000, transcendentals=40_000_000),
        name='attn_grads',
    )(q, d_out, stats, k_all, v_all)


def solution(mesh):
    cp_size = mesh.shape['cp']
    num_chips = cp_size // CORES
    swap_pairs = [(dev, dev ^ 1) for dev in range(cp_size)]
    core_groups = [[chip * CORES + core for chip in range(num_chips)] for core in range(CORES)]

    def local_grads(q_raw, k_raw, v_proj, out_fwd, lse_fwd, d_out, q_norm, k_norm):
        dev_rank = lax.axis_index('cp')
        core, chip = dev_rank % CORES, dev_rank // CORES
        local_rows, num_heads = q_raw.shape[0], q_raw.shape[1]
        chunk_len = local_rows // 2
        kv_heads = k_raw.shape[1]
        per_kv = num_heads // kv_heads
        half = kv_heads // CORES

        def by_head(arr):
            n = arr.shape[1] // kv_heads
            arr = arr.reshape((2, chunk_len, CORES, half, n) + arr.shape[2:])
            return jnp.moveaxis(arr, (2, 3, 0, 4, 1), (0, 1, 2, 3, 4))

        def swap(arr):
            mine = lax.dynamic_index_in_dim(arr, core, 0, False)
            theirs = lax.ppermute(lax.dynamic_index_in_dim(arr, 1 - core, 0, False), 'cp', swap_pairs)
            first = jnp.where(core == 0, mine, theirs)
            second = jnp.where(core == 0, theirs, mine)
            return jnp.stack([first[:, 0], second[:, 0], second[:, 1], first[:, 1]], axis=1)

        def unswap(arr):
            first = jnp.stack([arr[:, 0], arr[:, 3]], axis=1)
            second = jnp.stack([arr[:, 1], arr[:, 2]], axis=1)
            mine = jnp.where(core == 0, first, second)
            theirs = lax.ppermute(jnp.where(core == 0, second, first), 'cp', swap_pairs)
            both = jnp.stack([jnp.where(core == 0, mine, theirs), jnp.where(core == 0, theirs, mine)])
            both = jnp.moveaxis(both, (2, 4, 0, 1, 3), (0, 1, 2, 3, 4))
            return both.reshape(local_rows, -1, HEAD_DIM)

        delta = jnp.sum(d_out.astype(jnp.float32) * out_fwd.astype(jnp.float32), axis=-1)
        stats = swap(by_head(jnp.stack([lse_fwd * LOG2E, delta], axis=-1)))
        stats = jnp.moveaxis(stats, -1, 2).reshape(half, 4, 2, per_kv * chunk_len)
        kv = swap(jnp.concatenate([by_head(k_raw), by_head(v_proj)], axis=3))
        q_x = swap(by_head(q_raw))
        do_x = swap(by_head(d_out)).reshape(half, 4, per_kv * chunk_len, HEAD_DIM)
        k_x, v_x = kv[:, :, 0], kv[:, :, 1]

        num_chunks = 2 * cp_size
        chunk_ids = jnp.stack([2 * chip, 2 * chip + 1, num_chunks - 2 - 2 * chip, num_chunks - 1 - 2 * chip])
        positions = chunk_ids[:, None] * chunk_len + jnp.arange(chunk_len)
        cos_t, sin_t = rope_tables(positions)
        q_full, pull_q = jax.vjp(lambda a, w: norm_rope(a, w, cos_t[None, :, None], sin_t[None, :, None]), q_x.astype(jnp.float32), q_norm)
        k_full, pull_k = jax.vjp(lambda a, w: norm_rope(a, w, cos_t[None], sin_t[None]), k_x.astype(jnp.float32), k_norm)
        q_b = q_full.astype(jnp.bfloat16).reshape(half, 4, per_kv * chunk_len, HEAD_DIM)
        k_b = k_full.astype(jnp.bfloat16)
        k_all = lax.all_gather(k_b, 'cp', axis_index_groups=core_groups)
        v_all = lax.all_gather(v_x, 'cp', axis_index_groups=core_groups)
        dq, dk_parts, dv_parts = attn_grads(q_b, do_x, stats, k_all, v_all)
        dk = lax.psum_scatter(dk_parts, 'cp', axis_index_groups=core_groups) * SM_SCALE
        dv = lax.psum_scatter(dv_parts, 'cp', axis_index_groups=core_groups)
        dq_raw, dq_weight = pull_q(dq)
        dk_raw, dk_weight = pull_k(dk)
        weights = lax.psum(jnp.stack([dq_weight, dk_weight]), 'cp')
        dkv = unswap(jnp.stack([dk_raw.astype(jnp.bfloat16), dv.astype(jnp.bfloat16)], axis=2))
        dkv = dkv.reshape(local_rows, kv_heads, 2, HEAD_DIM)
        return (unswap(dq_raw.astype(jnp.bfloat16)), dkv[:, :, 0], dkv[:, :, 1], weights[0], weights[1])

    row_spec = P(('dp', 'cp'))
    in_specs = (row_spec, row_spec, row_spec, row_spec, row_spec, row_spec, P(), P())
    out_specs = (row_spec, row_spec, row_spec, P('dp'), P('dp'))
    return jax.shard_map(local_grads, mesh=mesh, in_specs=in_specs, out_specs=out_specs, check_vma=False)
```

```python
import functools

import jax
import jax.numpy as jnp
from jax import lax
from jax.experimental import pallas as pl
from jax.experimental.pallas import tpu as pltpu
from jax.sharding import PartitionSpec as P

HEAD_DIM = 128
ROPE_THETA = 1000000.0
NORM_EPS = 1e-6
LOG2E = 1.4426950408889634
SM_SCALE = HEAD_DIM ** -0.5
CORES = 2
MESH = pl.DeviceIdType.MESH


def rope_tables(positions):
    inv_freq = ROPE_THETA ** (-jnp.arange(0, HEAD_DIM, 2).astype(jnp.float32) / HEAD_DIM)
    angles = positions.astype(jnp.float32)[..., None] * inv_freq
    cos_t, sin_t = jnp.cos(angles), jnp.sin(angles)
    return jnp.concatenate([cos_t, cos_t], axis=-1), jnp.concatenate([-sin_t, sin_t], axis=-1)


def swap_halves(arr):
    return pltpu.roll(arr, HEAD_DIM // 2, arr.ndim - 1)


def inverse_rms(raw_in):
    return lax.rsqrt(jnp.mean(raw_in * raw_in, axis=-1, keepdims=True) + NORM_EPS)


def norm_rope_pull(raw_in, weight, cos_t, sin_t, grad):
    inv_rms = inverse_rms(raw_in)
    unit = raw_in * inv_rms
    grad_normed = grad * cos_t - swap_halves(grad) * sin_t
    weight_terms = grad_normed * unit
    grad_unit = grad_normed * weight
    grad_raw = inv_rms * (grad_unit - unit * jnp.mean(grad_unit * unit, axis=-1, keepdims=True))
    return grad_raw, weight_terms.reshape(-1, 8, HEAD_DIM).sum(0)


def dot(a, b):
    return lax.dot_general(a, b, (((1,), (0,)), ((), ())), preferred_element_type=jnp.float32)


def attn_kernel(num_chips, q_hbm, do_hbm, st_hbm, kv_hbm, k_raw, cos_q, sin_q, cos_k, sin_k, wq, wk,
                dq_hbm, dk_out, dv_out, dw_out,
                q_buf, do_buf, st_buf, kv_buf, q_now, qt_now, dot_now, dqt_now, kt_now, p_now, ds_now,
                acc, own_acc, own_recv, send_buf, transit, part, total, dw_acc, dw_all,
                ex_send, ex_recv, ex_local, own_send, own_kv_recv, own_local, nb_send, nb_recv, rl_send, op_recv,
                pt_send, pt_recv, tr_send, tr_recv, fw_send, fw_recv, oa_send, oa_recv,
                dq_send, dq_recv, dq_local, dw_send, dw_recv):
    me = lax.axis_index('cp')
    chip, core = me // CORES, me % CORES
    left, right = (chip + num_chips - 1) % num_chips, (chip + 1) % num_chips
    far = (chip + 2) % num_chips
    heads = q_buf.shape[0]
    num_chunks, chunk_len = kv_buf.shape[2], kv_buf.shape[4]
    per_kv = q_buf.shape[2] // chunk_len

    def remote(src, dst, send_sem, recv_sem, to_chip, to_core):
        return pltpu.make_async_remote_copy(src_ref=src, dst_ref=dst, send_sem=send_sem, recv_sem=recv_sem,
                                            device_id={'cp': to_chip * CORES + to_core}, device_id_type=MESH)

    def place(of_core, ch):
        return of_core if ch == 0 else num_chunks - 1 - of_core

    exchanged = ((q_hbm, q_buf), (do_hbm, do_buf), (st_hbm, st_buf))

    def ex_copies(h):
        for a, (src, dst) in enumerate(exchanged):
            for ch in range(2):
                mine = place(core, ch)
                yield (remote(src.at[(1 - core) * heads + h, ch], dst.at[h, mine], ex_send.at[h, a, ch], ex_recv.at[h, a, ch], chip, 1 - core),
                       remote(src.at[(1 - core) * heads + h, ch], dst.at[h, place(1 - core, ch)], ex_send.at[h, a, ch], ex_recv.at[h, a, ch], chip, 1 - core),
                       pltpu.make_async_copy(src.at[core * heads + h, ch], dst.at[h, mine], ex_local.at[h, a, ch]))

    def own_copies(h):
        for ch in range(2):
            mine = place(core, ch)
            yield (remote(kv_hbm.at[(1 - core) * heads + h, ch], kv_buf.at[0, h, mine], own_send.at[h, ch], own_kv_recv.at[h, ch], chip, 1 - core),
                   remote(kv_hbm.at[(1 - core) * heads + h, ch], kv_buf.at[0, h, place(1 - core, ch)], own_send.at[h, ch], own_kv_recv.at[h, ch], chip, 1 - core),
                   pltpu.make_async_copy(kv_hbm.at[core * heads + h, ch], kv_buf.at[0, h, mine], own_local.at[h, ch]))

    def nb_out(h, to_core, ch, way):
        return remote(kv_hbm.at[to_core * heads + h, ch], kv_buf.at[3 if way == 0 else 1, h, place(core, ch)],
                      nb_send.at[h, to_core, ch, way], nb_recv.at[h, place(core, ch), way], right if way == 0 else left, to_core)

    def second_sent(way):
        return chip >= 2 if way == 0 else chip >= 1

    def nb_each(h, fn):
        for way in range(2):
            for to_core in range(CORES):
                fn(nb_out(h, to_core, 0, way))

            @pl.when(second_sent(way))
            def _():
                for to_core in range(CORES):
                    fn(nb_out(h, to_core, 1, way))

    def nb_wait(h, way):
        slot = 3 if way == 0 else 1

        def wait(idx):
            remote(kv_hbm.at[0, 0], kv_buf.at[slot, h, idx], nb_send.at[h, 0, 0, way], nb_recv.at[h, idx, way], left, core).wait_recv()

        wait(0)
        wait(1)

        @pl.when(left >= 2 if way == 0 else right >= 1)
        def _():
            wait(2)
            wait(3)

    def relay(h, second, kind):
        src_slot, to_chip = (3, right) if kind == 0 else (1, left)
        pair = pl.ds(2 * second, 2)
        return remote(kv_buf.at[src_slot, h, pair, kind], kv_buf.at[2, h, pair, kind], rl_send.at[h, second, kind], op_recv.at[h, second, kind], to_chip, core)

    def relay_each(h, fn):
        for kind in range(2):
            fn(relay(h, 0, kind))

            @pl.when(right < left if kind == 0 else left < right)
            def _():
                fn(relay(h, 1, kind))

    def part_out(h, off, idx):
        to_chip = right if off == 1 else left
        home_core = idx if idx < 2 else num_chunks - 1 - idx
        return remote(send_buf.at[h, off - 1, idx], part.at[2 if off == 1 else 0, core * heads + h, idx // 2],
                      pt_send.at[h, off // 2, idx], pt_recv.at[1 if off == 1 else 0, core * heads + h, idx // 2], to_chip, home_core)

    def transit_out(h, second, kind):
        pair = pl.ds(2 * second, 2)
        return remote(send_buf.at[h, 1, pair, kind], transit.at[h, kind, pair], tr_send.at[h, second, kind], tr_recv.at[h, second, kind],
                      right if kind == 0 else left, core)

    def forward_out(h, idx, kind):
        home_core = idx if idx < 2 else num_chunks - 1 - idx
        return remote(transit.at[h, kind, idx], part.at[1, core * heads + h, idx // 2, kind],
                      fw_send.at[h, idx, kind], fw_recv.at[core * heads + h, idx // 2, kind], right if kind == 0 else left, home_core)

    def forward_each(h, fn):
        for kind in range(2):
            fn(h, 0, kind)

            @pl.when(left < right if kind == 0 else right < left)
            def _():
                fn(h, 1, kind)

    def start_forward(h, second, kind):
        transit_out(h, second, kind).wait_recv()
        for idx in (2 * second, 2 * second + 1):
            forward_out(h, idx, kind).start()

    def end_forward(h, second, kind):
        for idx in (2 * second, 2 * second + 1):
            forward_out(h, idx, kind).wait_send()

    def own_out(h, ch):
        return remote(own_acc.at[h, place(1 - core, ch)], own_recv.at[h, ch], oa_send.at[h, ch], oa_recv.at[h, ch], chip, 1 - core)

    def dq_copies(h):
        for ch in range(2):
            yield (remote(q_buf.at[h, place(1 - core, ch)], dq_hbm.at[core * heads + h, ch], dq_send.at[h, ch], dq_recv.at[h, ch], chip, 1 - core),
                   remote(q_buf.at[h, place(1 - core, ch)], dq_hbm.at[(1 - core) * heads + h, ch], dq_send.at[h, ch], dq_recv.at[h, ch], chip, 1 - core),
                   pltpu.make_async_copy(q_buf.at[h, place(core, ch)], dq_hbm.at[core * heads + h, ch], dq_local.at[h, ch]))

    def dw_out_to(step):
        peer = (me + step) % (num_chips * CORES)
        return remote(dw_acc, dw_all.at[me], dw_send.at[step], dw_recv.at[me], peer // CORES, peer % CORES)

    def block(h, off, kc, qb, masked):
        k_blk, v_blk = kv_buf[off, h, kc, 0], kv_buf[off, h, kc, 1]
        if masked:
            key_pos = lax.broadcasted_iota(jnp.int32, (chunk_len, chunk_len), 0)
            query_pos = lax.broadcasted_iota(jnp.int32, (chunk_len, chunk_len), 1)
            visible = key_pos <= query_pos
        for g in range(per_kv):
            cols = pl.ds(g * chunk_len, chunk_len)
            logits = dot(k_blk, qt_now[qb, :, cols]) * (SM_SCALE * LOG2E) - st_buf[h, qb, 0, g:g + 1, :]
            if masked:
                logits = jnp.where(visible, logits, -jnp.inf)
            prob = jnp.exp2(logits)
            dprob = dot(v_blk, dot_now[qb, :, cols])
            p_now[:, cols] = prob.astype(jnp.bfloat16)
            ds_now[:, cols] = (prob * (dprob - st_buf[h, qb, 1, g:g + 1, :])).astype(jnp.bfloat16)
        acc[kc, 1] += dot(p_now[...], do_buf[h, qb])
        acc[kc, 0] += dot(ds_now[...], q_now[qb])
        dqt_now[qb] += dot(kt_now[...], ds_now[...])

    def source_block(h, off):
        src = (chip + off) % num_chips
        own = off == 0
        early = src < chip
        acc[...] = jnp.zeros_like(acc)

        @pl.loop(0, jnp.where(early, num_chunks // 2, num_chunks))
        def _(kc):
            kt_now[...] = kv_buf[off, h, kc, 0].T

            @pl.when(own)
            def _():
                block(h, off, kc, kc, True)

            @pl.loop(jnp.where(own, kc + 1, jnp.where(early, 0, num_chunks // 2)), num_chunks)
            def _(qb):
                block(h, off, kc, qb, False)

    barrier = pltpu.get_barrier_semaphore()
    for step in range(1, num_chips * CORES):
        pl.semaphore_signal(barrier, inc=1, device_id={'cp': (me + step) % (num_chips * CORES)}, device_id_type=MESH)
    pl.semaphore_wait(barrier, num_chips * CORES - 1)

    nb_each(0, lambda copy: copy.start())

    @pl.loop(0, heads)
    def _(h):
        for out, _, local in own_copies(h):
            out.start()
            local.start()
        for out, _, local in ex_copies(h):
            out.start()
            local.start()

    dw_acc[...] = jnp.zeros_like(dw_acc)

    @pl.loop(0, heads)
    def _(h):
        for copies in (own_copies(h), ex_copies(h)):
            for out, arriving, local in copies:
                out.wait_send()
                arriving.wait_recv()
                local.wait()
        dqt_now[...] = jnp.zeros_like(dqt_now)

        @pl.loop(0, num_chunks)
        def _(qb):
            for g in range(per_kv):
                rows = pl.ds(g * chunk_len, chunk_len)
                raw = q_buf[h, qb, rows, :].astype(jnp.float32)
                normed = raw * inverse_rms(raw) * wq[...]
                query = (normed * cos_q[qb] + swap_halves(normed) * sin_q[qb]).astype(jnp.bfloat16)
                q_now[qb, rows, :] = query
                qt_now[qb, :, rows] = query.T
            dot_now[qb] = do_buf[h, qb].T

        last = h == heads - 1

        @pl.loop(0, num_chips)
        def _(j):
            first_order = jnp.where(j == 0, 0, jnp.where(j == 1, 1, jnp.where(j == 2, 3, 2)))
            last_order = jnp.where(j == 0, 2, jnp.where(j == 1, 1, jnp.where(j == 2, 3, 0)))
            off = jnp.where(last, last_order, first_order)

            @pl.when(off == 2)
            def _():
                for kind in range(2):
                    relay(h, 0, kind).wait_recv()

                @pl.when(chip < far)
                def _():
                    for kind in range(2):
                        relay(h, 1, kind).wait_recv()

            source_block(h, off)
            src = (chip + off) % num_chips

            @pl.when(off == 0)
            def _():
                own_acc[h] = acc[...]
                for ch in range(2):
                    own_out(h, ch).start()

            @pl.when(off != 0)
            def _():
                send_buf[h, off - 1, 0:2] = acc[0:2].astype(jnp.bfloat16)

                @pl.when(chip < src)
                def _():
                    send_buf[h, off - 1, 2:4] = acc[2:4].astype(jnp.bfloat16)

            for side in (1, 3):
                @pl.when(off == side)
                def _():
                    part_out(h, side, 0).start()
                    part_out(h, side, 1).start()

                    @pl.when(chip < src)
                    def _():
                        part_out(h, side, 2).start()
                        part_out(h, side, 3).start()

            @pl.when(off == 2)
            def _():
                for kind in range(2):
                    transit_out(h, 0, kind).start()

                @pl.when(chip < src)
                def _():
                    for kind in range(2):
                        transit_out(h, 1, kind).start()

            def pass_keys(of_head):
                nb_wait(of_head, 0)
                nb_wait(of_head, 1)
                relay_each(of_head, lambda copy: copy.start())

                @pl.when(of_head + 1 < heads)
                def _():
                    nb_each(of_head + 1, lambda copy: copy.start())

            @pl.when((h == 0) & (j == 0))
            def _():
                pass_keys(0)

            @pl.when((j == 2) & (h + 1 < heads))
            def _():
                pass_keys(h + 1)

            @pl.when((j == 0) & (h > 0))
            def _():
                forward_each(h - 1, start_forward)

            @pl.when((j == 2) & last)
            def _():
                forward_each(h, start_forward)

        @pl.loop(0, num_chunks)
        def _(qb):
            for g in range(per_kv):
                rows = pl.ds(g * chunk_len, chunk_len)
                grad = dqt_now[qb, :, rows].T * SM_SCALE
                raw = q_buf[h, qb, rows, :].astype(jnp.float32)
                grad_raw, terms = norm_rope_pull(raw, wq[...], cos_q[qb], sin_q[qb], grad)
                q_buf[h, qb, rows, :] = grad_raw.astype(jnp.bfloat16)
                dw_acc[0] += terms

        for out, _, local in dq_copies(h):
            out.start()
            local.start()

    def home(head, h, own):
        for ch in range(2):
            mine = place(core, ch)
            total[...] = own_acc[h, mine] if own else own_recv[h, ch]

            def add(slot):
                total[...] += part[slot, head, ch].astype(jnp.float32)

            def take_side(way):
                remote(send_buf.at[0, 0, 0], part.at[2 * way, head, ch], pt_send.at[0, 0, 0], pt_recv.at[way, head, ch], left, core).wait_recv()
                add(2 * way)

            def take_far():
                for kind in range(2):
                    remote(transit.at[0, 0, 0], part.at[1, head, ch, kind], fw_send.at[0, 0, 0], fw_recv.at[head, ch, kind], left, core).wait_recv()
                add(1)

            if ch == 0:
                take_side(0)
                take_side(1)
                take_far()
            else:
                @pl.when(right < chip)
                def _():
                    take_side(0)

                @pl.when(left < chip)
                def _():
                    take_side(1)

                @pl.when(far < chip)
                def _():
                    take_far()

            raw = k_raw[head, ch].astype(jnp.float32)
            grad_raw, terms = norm_rope_pull(raw, wk[...], cos_k[ch], sin_k[ch], total[0] * SM_SCALE)
            dk_out[head, ch] = grad_raw.astype(jnp.bfloat16)
            dv_out[head, ch] = total[1].astype(jnp.bfloat16)
            dw_acc[1] += terms

    @pl.loop(0, heads)
    def _(h):
        for ch in range(2):
            own_out(h, ch).wait_recv()
            own_out(h, ch).wait_send()
        home((1 - core) * heads + h, h, False)
        home(core * heads + h, h, True)

    for step in range(1, num_chips * CORES):
        dw_out_to(step).start()
    dw_all[me] = dw_acc[...]

    @pl.loop(0, heads)
    def _(h):
        nb_each(h, lambda copy: copy.wait_send())
        relay_each(h, lambda copy: copy.wait_send())
        for off in (1, 3):
            part_out(h, off, 0).wait_send()
            part_out(h, off, 1).wait_send()

            @pl.when(chip < (chip + off) % num_chips)
            def _():
                part_out(h, off, 2).wait_send()
                part_out(h, off, 3).wait_send()
        for kind in range(2):
            transit_out(h, 0, kind).wait_send()

        @pl.when(chip < far)
        def _():
            for kind in range(2):
                transit_out(h, 1, kind).wait_send()
        forward_each(h, end_forward)
        for out, arriving, local in dq_copies(h):
            out.wait_send()
            arriving.wait_recv()
            local.wait()

    for step in range(1, num_chips * CORES):
        peer = (me + step) % (num_chips * CORES)
        dw_out_to(step).wait_send()
        remote(dw_acc, dw_all.at[peer], dw_send.at[step], dw_recv.at[peer], chip, core).wait_recv()
    dw_out[...] = dw_all[...].sum(0).sum(1)


def attn_grads(num_chips, q, d_out, stats, kv, k_raw, cos_q, sin_q, cos_k, sin_k, wq, wk):
    kv_heads, _, rows, _ = q.shape
    chunk_len = kv.shape[3]
    heads = kv_heads // CORES
    half = (2, chunk_len, HEAD_DIM)
    bf16, f32 = jnp.bfloat16, jnp.float32
    sem = pltpu.SemaphoreType.DMA
    any_spec, vmem = pl.BlockSpec(memory_space=pl.ANY), pl.BlockSpec(memory_space=pltpu.VMEM)
    return pl.pallas_call(
        functools.partial(attn_kernel, num_chips),
        in_specs=[any_spec] * 4 + [vmem] * 7,
        out_specs=[any_spec, vmem, vmem, vmem],
        out_shape=[jax.ShapeDtypeStruct(q.shape, bf16), jax.ShapeDtypeStruct(k_raw.shape, bf16),
                   jax.ShapeDtypeStruct(k_raw.shape, bf16), jax.ShapeDtypeStruct((2, HEAD_DIM), f32)],
        scratch_shapes=[
            pltpu.VMEM((heads, 4, rows, HEAD_DIM), bf16),
            pltpu.VMEM((heads, 4, rows, HEAD_DIM), bf16),
            pltpu.VMEM((heads, 4) + stats.shape[2:], f32),
            pltpu.VMEM((num_chips, heads, 4) + half, bf16),
            pltpu.VMEM((4, rows, HEAD_DIM), bf16),
            pltpu.VMEM((4, HEAD_DIM, rows), bf16),
            pltpu.VMEM((4, HEAD_DIM, rows), bf16),
            pltpu.VMEM((4, HEAD_DIM, rows), f32),
            pltpu.VMEM((HEAD_DIM, chunk_len), bf16),
            pltpu.VMEM((chunk_len, rows), bf16),
            pltpu.VMEM((chunk_len, rows), bf16),
            pltpu.VMEM((4,) + half, f32),
            pltpu.VMEM((heads, 4) + half, f32),
            pltpu.VMEM((heads, 2) + half, f32),
            pltpu.VMEM((heads, 3, 4) + half, bf16),
            pltpu.VMEM((heads, 2, 4, chunk_len, HEAD_DIM), bf16),
            pltpu.VMEM((3, kv_heads, 2) + half, bf16),
            pltpu.VMEM(half, f32),
            pltpu.VMEM((2, 8, HEAD_DIM), f32),
            pltpu.VMEM((num_chips * CORES, 2, 8, HEAD_DIM), f32),
            sem((heads, 3, 2)), sem((heads, 3, 2)), sem((heads, 3, 2)),
            sem((heads, 2)), sem((heads, 2)), sem((heads, 2)),
            sem((heads, CORES, 2, 2)), sem((heads, 4, 2)),
            sem((heads, 2, 2)), sem((heads, 2, 2)),
            sem((heads, 2, 4)), sem((2, kv_heads, 2)),
            sem((heads, 2, 2)), sem((heads, 2, 2)),
            sem((heads, 4, 2)), sem((kv_heads, 2, 2)),
            sem((heads, 2)), sem((heads, 2)),
            sem((heads, 2)), sem((heads, 2)), sem((heads, 2)),
            sem((num_chips * CORES,)), sem((num_chips * CORES,)),
        ],
        compiler_params=pltpu.CompilerParams(vmem_limit_bytes=60 * 2 ** 20, collective_id=0, has_side_effects=True),
        cost_estimate=pl.CostEstimate(flops=50_000_000_000, bytes_accessed=64_000_000, transcendentals=40_000_000),
        name='attn_grads',
    )(q, d_out, stats, kv, k_raw, cos_q, sin_q, cos_k, sin_k, wq, wk)


def solution(mesh):
    cp_size = mesh.shape['cp']
    num_chips = cp_size // CORES

    def local_grads(q_raw, k_raw, v_proj, out_fwd, lse_fwd, d_out, q_norm, k_norm):
        dev_rank = lax.axis_index('cp')
        chip = dev_rank // CORES
        local_rows, num_heads = q_raw.shape[0], q_raw.shape[1]
        chunk_len = local_rows // 2
        kv_heads = k_raw.shape[1]
        per_kv = num_heads // kv_heads

        def by_head(arr):
            n = arr.shape[1] // kv_heads
            arr = arr.reshape((2, chunk_len, kv_heads, n) + arr.shape[2:])
            return jnp.moveaxis(arr, (2, 0, 3, 1), (0, 1, 2, 3))

        num_chunks = 2 * cp_size
        offsets = jnp.arange(chunk_len)
        chip_chunks = jnp.stack([2 * chip, 2 * chip + 1, num_chunks - 2 - 2 * chip, num_chunks - 1 - 2 * chip])
        cos_q, sin_q = rope_tables(chip_chunks[:, None] * chunk_len + offsets)
        dev_chunks = jnp.stack([dev_rank, num_chunks - 1 - dev_rank])
        cos_k, sin_k = rope_tables(dev_chunks[:, None] * chunk_len + offsets)

        delta = jnp.sum(d_out.astype(jnp.float32) * out_fwd.astype(jnp.float32), axis=-1)
        stats = jnp.stack([by_head(lse_fwd * LOG2E), by_head(delta)], axis=2)
        q_h = by_head(q_raw).reshape(kv_heads, 2, per_kv * chunk_len, HEAD_DIM)
        do_h = by_head(d_out).reshape(kv_heads, 2, per_kv * chunk_len, HEAD_DIM)
        k_h, v_h = by_head(k_raw)[:, :, 0], by_head(v_proj)[:, :, 0]
        raw = k_h.astype(jnp.float32)
        normed = raw * inverse_rms(raw) * k_norm
        key = normed * cos_k + jnp.concatenate([normed[..., HEAD_DIM // 2:], normed[..., :HEAD_DIM // 2]], axis=-1) * sin_k
        kv = jnp.stack([key.astype(jnp.bfloat16), v_h], axis=2)
        dq, dk, dv, weights = attn_grads(num_chips, q_h, do_h, stats, kv, k_h, cos_q, sin_q, cos_k, sin_k, q_norm[None], k_norm[None])

        def by_row(arr):
            arr = arr.reshape(kv_heads, 2, -1, chunk_len, HEAD_DIM)
            return jnp.moveaxis(arr, (1, 3, 0, 2), (0, 1, 2, 3)).reshape(local_rows, -1, HEAD_DIM)

        return by_row(dq), by_row(dk), by_row(dv), weights[0], weights[1]

    row_spec = P(('dp', 'cp'))
    in_specs = (row_spec, row_spec, row_spec, row_spec, row_spec, row_spec, P(), P())
    out_specs = (row_spec, row_spec, row_spec, P('dp'), P('dp'))
    return jax.shard_map(local_grads, mesh=mesh, in_specs=in_specs, out_specs=out_specs, check_vma=False)
```

```python
import functools

import jax
import jax.numpy as jnp
from jax import lax
from jax.experimental import pallas as pl
from jax.experimental.pallas import tpu as pltpu
from jax.sharding import PartitionSpec as P

HEAD_DIM = 128
ROPE_THETA = 1000000.0
NORM_EPS = 1e-6
LOG2E = 1.4426950408889634
SM_SCALE = HEAD_DIM ** -0.5
CORES = 2
MESH = pl.DeviceIdType.MESH


def rope_tables(positions):
    inv_freq = ROPE_THETA ** (-jnp.arange(0, HEAD_DIM, 2).astype(jnp.float32) / HEAD_DIM)
    angles = positions.astype(jnp.float32)[..., None] * inv_freq
    cos_t, sin_t = jnp.cos(angles), jnp.sin(angles)
    return jnp.concatenate([cos_t, cos_t], axis=-1), jnp.concatenate([-sin_t, sin_t], axis=-1)


def swap_halves(arr):
    return pltpu.roll(arr, HEAD_DIM // 2, arr.ndim - 1)


def inverse_rms(raw_in):
    return lax.rsqrt(jnp.mean(raw_in * raw_in, axis=-1, keepdims=True) + NORM_EPS)


def norm_rope_pull(raw_in, weight, cos_t, sin_t, grad):
    inv_rms = inverse_rms(raw_in)
    unit = raw_in * inv_rms
    grad_normed = grad * cos_t - swap_halves(grad) * sin_t
    weight_terms = grad_normed * unit
    grad_unit = grad_normed * weight
    grad_raw = inv_rms * (grad_unit - unit * jnp.mean(grad_unit * unit, axis=-1, keepdims=True))
    return grad_raw, weight_terms.reshape(-1, 8, HEAD_DIM).sum(0)


def swap_rows(arr):
    return jnp.concatenate([arr[HEAD_DIM // 2:], arr[:HEAD_DIM // 2]], axis=0)


def inverse_rms_t(raw_in):
    return lax.rsqrt(jnp.mean(raw_in * raw_in, axis=0, keepdims=True) + NORM_EPS)


def dot(a, b):
    return lax.dot_general(a, b, (((1,), (0,)), ((), ())), preferred_element_type=jnp.float32)


def attn_kernel(num_chips, q_hbm, do_hbm, st_hbm, kv_hbm, k_raw, cos_q, sin_q, cos_k, sin_k, wq, wk,
                dq_hbm, dk_out, dv_out, dw_out,
                q_buf, do_buf, st_buf, kv_buf, raw_now, q_now, qt_now, dot_now, dqt_now, kt_now, p_now, ds_now,
                acc, own_acc, own_recv, send_buf, transit, part, total, dwq_acc, dw_acc, dw_all,
                ex_send, ex_recv, ex_local, own_send, own_kv_recv, own_local, nb_send, nb_recv, rl_send, op_recv,
                pt_send, pt_recv, tr_send, tr_recv, fw_send, fw_recv, oa_send, oa_recv,
                dq_send, dq_recv, dq_local, dw_send, dw_recv):
    me = lax.axis_index('cp')
    chip, core = me // CORES, me % CORES
    left, right = (chip + num_chips - 1) % num_chips, (chip + 1) % num_chips
    far = (chip + 2) % num_chips
    heads = q_buf.shape[0]
    num_chunks, chunk_len = kv_buf.shape[2], kv_buf.shape[4]
    per_kv = q_buf.shape[2] // chunk_len

    def remote(src, dst, send_sem, recv_sem, to_chip, to_core):
        return pltpu.make_async_remote_copy(src_ref=src, dst_ref=dst, send_sem=send_sem, recv_sem=recv_sem,
                                            device_id={'cp': to_chip * CORES + to_core}, device_id_type=MESH)

    def place(of_core, ch):
        return of_core if ch == 0 else num_chunks - 1 - of_core

    exchanged = ((q_hbm, q_buf), (do_hbm, do_buf), (st_hbm, st_buf))

    def ex_copies(h):
        for a, (src, dst) in enumerate(exchanged):
            for ch in range(2):
                mine = place(core, ch)
                yield (remote(src.at[(1 - core) * heads + h, ch], dst.at[h, mine], ex_send.at[h, a, ch], ex_recv.at[h, a, ch], chip, 1 - core),
                       remote(src.at[(1 - core) * heads + h, ch], dst.at[h, place(1 - core, ch)], ex_send.at[h, a, ch], ex_recv.at[h, a, ch], chip, 1 - core),
                       pltpu.make_async_copy(src.at[core * heads + h, ch], dst.at[h, mine], ex_local.at[h, a, ch]))

    def own_copies(h):
        for ch in range(2):
            mine = place(core, ch)
            yield (remote(kv_hbm.at[(1 - core) * heads + h, ch], kv_buf.at[0, h, mine], own_send.at[h, ch], own_kv_recv.at[h, ch], chip, 1 - core),
                   remote(kv_hbm.at[(1 - core) * heads + h, ch], kv_buf.at[0, h, place(1 - core, ch)], own_send.at[h, ch], own_kv_recv.at[h, ch], chip, 1 - core),
                   pltpu.make_async_copy(kv_hbm.at[core * heads + h, ch], kv_buf.at[0, h, mine], own_local.at[h, ch]))

    def nb_out(h, to_core, ch, way):
        return remote(kv_hbm.at[to_core * heads + h, ch], kv_buf.at[3 if way == 0 else 1, h, place(core, ch)],
                      nb_send.at[h, to_core, ch, way], nb_recv.at[h, place(core, ch), way], right if way == 0 else left, to_core)

    def second_sent(way):
        return chip >= 2 if way == 0 else chip >= 1

    def nb_each(h, fn):
        for way in range(2):
            for to_core in range(CORES):
                fn(nb_out(h, to_core, 0, way))

            @pl.when(second_sent(way))
            def _():
                for to_core in range(CORES):
                    fn(nb_out(h, to_core, 1, way))

    def nb_wait(h, way):
        slot = 3 if way == 0 else 1

        def wait(idx):
            remote(kv_hbm.at[0, 0], kv_buf.at[slot, h, idx], nb_send.at[h, 0, 0, way], nb_recv.at[h, idx, way], left, core).wait_recv()

        wait(0)
        wait(1)

        @pl.when(left >= 2 if way == 0 else right >= 1)
        def _():
            wait(2)
            wait(3)

    def relay(h, second, kind):
        src_slot, to_chip = (3, right) if kind == 0 else (1, left)
        pair = pl.ds(2 * second, 2)
        return remote(kv_buf.at[src_slot, h, pair, kind], kv_buf.at[2, h, pair, kind], rl_send.at[h, second, kind], op_recv.at[h, second, kind], to_chip, core)

    def relay_each(h, fn):
        for kind in range(2):
            fn(relay(h, 0, kind))

            @pl.when(right < left if kind == 0 else left < right)
            def _():
                fn(relay(h, 1, kind))

    def part_out(h, off, idx):
        to_chip = right if off == 1 else left
        home_core = idx if idx < 2 else num_chunks - 1 - idx
        return remote(send_buf.at[h, off - 1, idx], part.at[2 if off == 1 else 0, core * heads + h, idx // 2],
                      pt_send.at[h, off // 2, idx], pt_recv.at[1 if off == 1 else 0, core * heads + h, idx // 2], to_chip, home_core)

    def transit_out(h, second, kind):
        pair = pl.ds(2 * second, 2)
        return remote(send_buf.at[h, 1, pair, kind], transit.at[h, kind, pair], tr_send.at[h, second, kind], tr_recv.at[h, second, kind],
                      right if kind == 0 else left, core)

    def forward_out(h, idx, kind):
        home_core = idx if idx < 2 else num_chunks - 1 - idx
        return remote(transit.at[h, kind, idx], part.at[1, core * heads + h, idx // 2, kind],
                      fw_send.at[h, idx, kind], fw_recv.at[core * heads + h, idx // 2, kind], right if kind == 0 else left, home_core)

    def forward_each(h, fn):
        for kind in range(2):
            fn(h, 0, kind)

            @pl.when(left < right if kind == 0 else right < left)
            def _():
                fn(h, 1, kind)

    def start_forward(h, second, kind):
        transit_out(h, second, kind).wait_recv()
        for idx in (2 * second, 2 * second + 1):
            forward_out(h, idx, kind).start()

    def end_forward(h, second, kind):
        for idx in (2 * second, 2 * second + 1):
            forward_out(h, idx, kind).wait_send()

    def own_out(h, ch):
        return remote(own_acc.at[h, place(1 - core, ch)], own_recv.at[h, ch], oa_send.at[h, ch], oa_recv.at[h, ch], chip, 1 - core)

    def dq_copies(h):
        for ch in range(2):
            yield (remote(q_buf.at[h, place(1 - core, ch)], dq_hbm.at[core * heads + h, ch], dq_send.at[h, ch], dq_recv.at[h, ch], chip, 1 - core),
                   remote(q_buf.at[h, place(1 - core, ch)], dq_hbm.at[(1 - core) * heads + h, ch], dq_send.at[h, ch], dq_recv.at[h, ch], chip, 1 - core),
                   pltpu.make_async_copy(q_buf.at[h, place(core, ch)], dq_hbm.at[core * heads + h, ch], dq_local.at[h, ch]))

    def dw_out_to(step):
        peer = (me + step) % (num_chips * CORES)
        return remote(dw_acc, dw_all.at[me], dw_send.at[step], dw_recv.at[me], peer // CORES, peer % CORES)

    def block(h, off, kc, qb, masked):
        k_blk, v_blk = kv_buf[off, h, kc, 0], kv_buf[off, h, kc, 1]
        if masked:
            key_pos = lax.broadcasted_iota(jnp.int32, (chunk_len, chunk_len), 0)
            query_pos = lax.broadcasted_iota(jnp.int32, (chunk_len, chunk_len), 1)
            visible = key_pos <= query_pos
        for g in range(per_kv):
            cols = pl.ds(g * chunk_len, chunk_len)
            logits = dot(k_blk, qt_now[qb, :, cols]) * (SM_SCALE * LOG2E) - st_buf[h, qb, 0, g:g + 1, :]
            if masked:
                logits = jnp.where(visible, logits, -jnp.inf)
            prob = jnp.exp2(logits)
            dprob = dot(v_blk, dot_now[qb, :, cols])
            p_now[:, cols] = prob.astype(jnp.bfloat16)
            ds_now[:, cols] = (prob * (dprob - st_buf[h, qb, 1, g:g + 1, :])).astype(jnp.bfloat16)
        acc[kc, 1] += dot(p_now[...], do_buf[h, qb])
        acc[kc, 0] += dot(ds_now[...], q_now[qb])
        dqt_now[qb] += dot(kt_now[...], ds_now[...])

    def source_block(h, off):
        src = (chip + off) % num_chips
        own = off == 0
        early = src < chip
        acc[...] = jnp.zeros_like(acc)

        @pl.loop(0, jnp.where(early, num_chunks // 2, num_chunks))
        def _(kc):
            kt_now[...] = kv_buf[off, h, kc, 0].T

            @pl.when(own)
            def _():
                block(h, off, kc, kc, True)

            @pl.loop(jnp.where(own, kc + 1, jnp.where(early, 0, num_chunks // 2)), num_chunks)
            def _(qb):
                block(h, off, kc, qb, False)

    def home(head, h, own):
        for ch in range(2):
            mine = place(core, ch)
            total[...] = own_acc[h, mine] if own else own_recv[h, ch]

            def add(slot):
                total[...] += part[slot, head, ch].astype(jnp.float32)

            def take_side(way):
                remote(send_buf.at[0, 0, 0], part.at[2 * way, head, ch], pt_send.at[0, 0, 0], pt_recv.at[way, head, ch], left, core).wait_recv()
                add(2 * way)

            def take_far():
                for kind in range(2):
                    remote(transit.at[0, 0, 0], part.at[1, head, ch, kind], fw_send.at[0, 0, 0], fw_recv.at[head, ch, kind], left, core).wait_recv()
                add(1)

            if ch == 0:
                take_side(0)
                take_side(1)
                take_far()
            else:
                @pl.when(right < chip)
                def _():
                    take_side(0)

                @pl.when(left < chip)
                def _():
                    take_side(1)

                @pl.when(far < chip)
                def _():
                    take_far()

            raw = k_raw[head, ch].astype(jnp.float32)
            grad_raw, terms = norm_rope_pull(raw, wk[...], cos_k[ch], sin_k[ch], total[0] * SM_SCALE)
            dk_out[head, ch] = grad_raw.astype(jnp.bfloat16)
            dv_out[head, ch] = total[1].astype(jnp.bfloat16)
            dw_acc[1] += terms

    def home_head(h):
        for ch in range(2):
            own_out(h, ch).wait_recv()
            own_out(h, ch).wait_send()
        home((1 - core) * heads + h, h, False)
        home(core * heads + h, h, True)

    def compute_head(h):
        for copies in (own_copies(h), ex_copies(h)):
            for out, arriving, local in copies:
                out.wait_send()
                arriving.wait_recv()
                local.wait()
        dqt_now[...] = jnp.zeros_like(dqt_now)

        @pl.loop(0, num_chunks)
        def _(qb):
            for g in range(per_kv):
                rows = pl.ds(g * chunk_len, chunk_len)
                raw_bf = q_buf[h, qb, rows, :].T
                raw_now[qb, :, rows] = raw_bf
                raw = raw_bf.astype(jnp.float32)
                normed = raw * inverse_rms_t(raw) * wq[...]
                query = (normed * cos_q[qb] + swap_rows(normed) * sin_q[qb]).astype(jnp.bfloat16)
                qt_now[qb, :, rows] = query
                q_now[qb, rows, :] = query.T
            dot_now[qb] = do_buf[h, qb].T

        last = h == heads - 1

        @pl.loop(0, num_chips)
        def _(j):
            first_order = jnp.where(j == 0, 0, jnp.where(j == 1, 1, jnp.where(j == 2, 3, 2)))
            last_order = jnp.where(j == 0, 2, jnp.where(j == 1, 1, jnp.where(j == 2, 3, 0)))
            off = jnp.where(last, last_order, first_order)

            @pl.when(off == 2)
            def _():
                for kind in range(2):
                    relay(h, 0, kind).wait_recv()

                @pl.when(chip < far)
                def _():
                    for kind in range(2):
                        relay(h, 1, kind).wait_recv()

            source_block(h, off)
            src = (chip + off) % num_chips

            @pl.when(off == 0)
            def _():
                own_acc[h] = acc[...]
                for ch in range(2):
                    own_out(h, ch).start()

            @pl.when(off != 0)
            def _():
                send_buf[h, off - 1, 0:2] = acc[0:2].astype(jnp.bfloat16)

                @pl.when(chip < src)
                def _():
                    send_buf[h, off - 1, 2:4] = acc[2:4].astype(jnp.bfloat16)

            for side in (1, 3):
                @pl.when(off == side)
                def _():
                    part_out(h, side, 0).start()
                    part_out(h, side, 1).start()

                    @pl.when(chip < src)
                    def _():
                        part_out(h, side, 2).start()
                        part_out(h, side, 3).start()

            @pl.when(off == 2)
            def _():
                for kind in range(2):
                    transit_out(h, 0, kind).start()

                @pl.when(chip < src)
                def _():
                    for kind in range(2):
                        transit_out(h, 1, kind).start()

            def pass_keys(of_head):
                nb_wait(of_head, 0)
                nb_wait(of_head, 1)
                relay_each(of_head, lambda copy: copy.start())

                @pl.when(of_head + 2 < heads)
                def _():
                    nb_each(of_head + 2, lambda copy: copy.start())

            @pl.when((h == 0) & (j == 0))
            def _():
                pass_keys(0)

            @pl.when((j == 3) & (h + 1 < heads))
            def _():
                pass_keys(h + 1)

            @pl.when((j == 0) & (h > 0))
            def _():
                forward_each(h - 1, start_forward)

            @pl.when((j == 2) & last)
            def _():
                forward_each(h, start_forward)

        @pl.loop(0, num_chunks)
        def _(qb):
            for g in range(per_kv):
                rows = pl.ds(g * chunk_len, chunk_len)
                grad = dqt_now[qb, :, rows] * SM_SCALE
                raw = raw_now[qb, :, rows].astype(jnp.float32)
                inv_rms = inverse_rms_t(raw)
                unit = raw * inv_rms
                grad_normed = grad * cos_q[qb] - swap_rows(grad) * sin_q[qb]
                dwq_acc[...] += grad_normed * unit
                grad_unit = grad_normed * wq[...]
                grad_raw = inv_rms * (grad_unit - unit * jnp.mean(grad_unit * unit, axis=0, keepdims=True))
                q_buf[h, qb, rows, :] = grad_raw.astype(jnp.bfloat16).T

        for out, _, local in dq_copies(h):
            out.start()
            local.start()

    barrier = pltpu.get_barrier_semaphore()
    for step in range(1, num_chips * CORES):
        pl.semaphore_signal(barrier, inc=1, device_id={'cp': (me + step) % (num_chips * CORES)}, device_id_type=MESH)
    pl.semaphore_wait(barrier, num_chips * CORES - 1)

    nb_each(0, lambda copy: copy.start())

    @pl.loop(0, heads)
    def _(h):
        for out, _, local in own_copies(h):
            out.start()
            local.start()
        for out, _, local in ex_copies(h):
            out.start()
            local.start()

    nb_each(1, lambda copy: copy.start())

    dw_acc[...] = jnp.zeros_like(dw_acc)
    dwq_acc[...] = jnp.zeros_like(dwq_acc)

    @pl.loop(0, heads + 2)
    def _(h):
        @pl.when(h < heads)
        def _():
            compute_head(h)

        @pl.when(h >= 2)
        def _():
            home_head(h - 2)

    dw_acc[0] = dwq_acc[...].T.reshape(-1, 8, HEAD_DIM).sum(0)
    for step in range(1, num_chips * CORES):
        dw_out_to(step).start()
    dw_all[me] = dw_acc[...]

    @pl.loop(0, heads)
    def _(h):
        nb_each(h, lambda copy: copy.wait_send())
        relay_each(h, lambda copy: copy.wait_send())
        for off in (1, 3):
            part_out(h, off, 0).wait_send()
            part_out(h, off, 1).wait_send()

            @pl.when(chip < (chip + off) % num_chips)
            def _():
                part_out(h, off, 2).wait_send()
                part_out(h, off, 3).wait_send()
        for kind in range(2):
            transit_out(h, 0, kind).wait_send()

        @pl.when(chip < far)
        def _():
            for kind in range(2):
                transit_out(h, 1, kind).wait_send()
        forward_each(h, end_forward)
        for out, arriving, local in dq_copies(h):
            out.wait_send()
            arriving.wait_recv()
            local.wait()

    for step in range(1, num_chips * CORES):
        peer = (me + step) % (num_chips * CORES)
        dw_out_to(step).wait_send()
        remote(dw_acc, dw_all.at[peer], dw_send.at[step], dw_recv.at[peer], chip, core).wait_recv()
    dw_out[...] = dw_all[...].sum(0).sum(1)


def prepare_kernel(q_ref, do_ref, out_ref, k_ref, v_ref, lse_ref, cos_k, sin_k, wk, q_out, do_out, st_out, kv_out, k_out):
    rows, num_heads = q_ref.shape[0], q_ref.shape[1]
    kv_heads = k_ref.shape[1]
    f32, bf16 = jnp.float32, jnp.bfloat16

    def by_head(arr):
        return jnp.swapaxes(arr, 0, 1)

    d_out = do_ref[...].astype(f32)
    q_out[:, 0] = by_head(q_ref[...].astype(f32)).astype(bf16).reshape(kv_heads, -1, rows, HEAD_DIM)
    do_out[:, 0] = by_head(d_out).astype(bf16).reshape(kv_heads, -1, rows, HEAD_DIM)
    delta = jnp.sum(d_out * out_ref[...].astype(f32), axis=-1)
    st_out[:, 0, 0] = (lse_ref[...] * LOG2E).T.reshape(kv_heads, -1, rows)
    st_out[:, 0, 1] = delta.T.reshape(kv_heads, -1, rows)
    raw = k_ref[...].astype(f32)
    normed = raw * inverse_rms(raw) * wk[...]
    key = normed * cos_k[0][:, None] + swap_halves(normed) * sin_k[0][:, None]
    kv_out[:, 0, 0] = by_head(key).astype(bf16)
    kv_out[:, 0, 1] = by_head(v_ref[...].astype(f32)).astype(bf16)
    k_out[:, 0] = by_head(raw).astype(bf16)


def prepare(q_raw, d_out, out_fwd, k_raw, v_proj, lse_fwd, cos_k, sin_k, wk, rows=128):
    local_rows, num_heads, _ = q_raw.shape
    kv_heads = k_raw.shape[1]
    per_kv, chunk_len = num_heads // kv_heads, local_rows // 2
    parts = chunk_len // rows
    bf16 = jnp.bfloat16
    rows_q = pl.BlockSpec((rows, num_heads, HEAD_DIM), lambda i: (i, 0, 0))
    rows_k = pl.BlockSpec((rows, kv_heads, HEAD_DIM), lambda i: (i, 0, 0))
    table = pl.BlockSpec((1, rows, HEAD_DIM), lambda i: (i // parts, i % parts, 0))
    heads_q = pl.BlockSpec((kv_heads, 1, per_kv, rows, HEAD_DIM), lambda i: (0, i // parts, 0, i % parts, 0))
    return pl.pallas_call(
        prepare_kernel,
        grid=(2 * parts,),
        in_specs=[rows_q, rows_q, rows_q, rows_k, rows_k, pl.BlockSpec((rows, num_heads), lambda i: (i, 0)), table, table,
                  pl.BlockSpec((1, HEAD_DIM), lambda i: (0, 0))],
        out_specs=[heads_q, heads_q,
                   pl.BlockSpec((kv_heads, 1, 2, per_kv, rows), lambda i: (0, i // parts, 0, 0, i % parts)),
                   pl.BlockSpec((kv_heads, 1, 2, rows, HEAD_DIM), lambda i: (0, i // parts, 0, i % parts, 0)),
                   pl.BlockSpec((kv_heads, 1, rows, HEAD_DIM), lambda i: (0, i // parts, i % parts, 0))],
        out_shape=[jax.ShapeDtypeStruct((kv_heads, 2, per_kv, chunk_len, HEAD_DIM), bf16),
                   jax.ShapeDtypeStruct((kv_heads, 2, per_kv, chunk_len, HEAD_DIM), bf16),
                   jax.ShapeDtypeStruct((kv_heads, 2, 2, per_kv, chunk_len), jnp.float32),
                   jax.ShapeDtypeStruct((kv_heads, 2, 2, chunk_len, HEAD_DIM), bf16),
                   jax.ShapeDtypeStruct((kv_heads, 2, chunk_len, HEAD_DIM), bf16)],
        compiler_params=pltpu.CompilerParams(vmem_limit_bytes=48 * 2 ** 20),
        name='prepare',
    )(q_raw, d_out, out_fwd, k_raw, v_proj, lse_fwd, cos_k, sin_k, wk)


def finish_kernel(dq_ref, dk_ref, dv_ref, dq_out, dk_out, dv_out):
    for src, dst in ((dq_ref, dq_out), (dk_ref, dk_out), (dv_ref, dv_out)):
        by_head = src[:, 0].reshape(-1, src.shape[-2], HEAD_DIM).astype(jnp.float32)
        dst[...] = jnp.swapaxes(by_head, 0, 1).astype(jnp.bfloat16)


def finish(dq, dk, dv, rows=128):
    kv_heads, _, per_kv, chunk_len, _ = dq.shape
    parts = chunk_len // rows
    num_heads = kv_heads * per_kv
    heads_k = pl.BlockSpec((kv_heads, 1, rows, HEAD_DIM), lambda i: (0, i // parts, i % parts, 0))
    rows_k = pl.BlockSpec((rows, kv_heads, HEAD_DIM), lambda i: (i, 0, 0))
    out_k = jax.ShapeDtypeStruct((2 * chunk_len, kv_heads, HEAD_DIM), jnp.bfloat16)
    return pl.pallas_call(
        finish_kernel,
        grid=(2 * parts,),
        in_specs=[pl.BlockSpec((kv_heads, 1, per_kv, rows, HEAD_DIM), lambda i: (0, i // parts, 0, i % parts, 0)), heads_k, heads_k],
        out_specs=[pl.BlockSpec((rows, num_heads, HEAD_DIM), lambda i: (i, 0, 0)), rows_k, rows_k],
        out_shape=[jax.ShapeDtypeStruct((2 * chunk_len, num_heads, HEAD_DIM), jnp.bfloat16), out_k, out_k],
        compiler_params=pltpu.CompilerParams(vmem_limit_bytes=48 * 2 ** 20),
        name='finish',
    )(dq, dk, dv)


def attn_grads(num_chips, q, d_out, stats, kv, k_raw, cos_q, sin_q, cos_k, sin_k, wq, wk):
    kv_heads, _, rows, _ = q.shape
    chunk_len = kv.shape[3]
    heads = kv_heads // CORES
    half = (2, chunk_len, HEAD_DIM)
    bf16, f32 = jnp.bfloat16, jnp.float32
    sem = pltpu.SemaphoreType.DMA
    any_spec, vmem = pl.BlockSpec(memory_space=pl.ANY), pl.BlockSpec(memory_space=pltpu.VMEM)
    return pl.pallas_call(
        functools.partial(attn_kernel, num_chips),
        in_specs=[any_spec] * 4 + [vmem] * 7,
        out_specs=[any_spec, vmem, vmem, vmem],
        out_shape=[jax.ShapeDtypeStruct(q.shape, bf16), jax.ShapeDtypeStruct(k_raw.shape, bf16),
                   jax.ShapeDtypeStruct(k_raw.shape, bf16), jax.ShapeDtypeStruct((2, HEAD_DIM), f32)],
        scratch_shapes=[
            pltpu.VMEM((heads, 4, rows, HEAD_DIM), bf16),
            pltpu.VMEM((heads, 4, rows, HEAD_DIM), bf16),
            pltpu.VMEM((heads, 4) + stats.shape[2:], f32),
            pltpu.VMEM((num_chips, heads, 4) + half, bf16),
            pltpu.VMEM((4, HEAD_DIM, rows), bf16),
            pltpu.VMEM((4, rows, HEAD_DIM), bf16),
            pltpu.VMEM((4, HEAD_DIM, rows), bf16),
            pltpu.VMEM((4, HEAD_DIM, rows), bf16),
            pltpu.VMEM((4, HEAD_DIM, rows), f32),
            pltpu.VMEM((HEAD_DIM, chunk_len), bf16),
            pltpu.VMEM((chunk_len, rows), bf16),
            pltpu.VMEM((chunk_len, rows), bf16),
            pltpu.VMEM((4,) + half, f32),
            pltpu.VMEM((heads, 4) + half, f32),
            pltpu.VMEM((heads, 2) + half, f32),
            pltpu.VMEM((heads, 3, 4) + half, bf16),
            pltpu.VMEM((heads, 2, 4, chunk_len, HEAD_DIM), bf16),
            pltpu.VMEM((3, kv_heads, 2) + half, bf16),
            pltpu.VMEM(half, f32),
            pltpu.VMEM((HEAD_DIM, chunk_len), f32),
            pltpu.VMEM((2, 8, HEAD_DIM), f32),
            pltpu.VMEM((num_chips * CORES, 2, 8, HEAD_DIM), f32),
            sem((heads, 3, 2)), sem((heads, 3, 2)), sem((heads, 3, 2)),
            sem((heads, 2)), sem((heads, 2)), sem((heads, 2)),
            sem((heads, CORES, 2, 2)), sem((heads, 4, 2)),
            sem((heads, 2, 2)), sem((heads, 2, 2)),
            sem((heads, 2, 4)), sem((2, kv_heads, 2)),
            sem((heads, 2, 2)), sem((heads, 2, 2)),
            sem((heads, 4, 2)), sem((kv_heads, 2, 2)),
            sem((heads, 2)), sem((heads, 2)),
            sem((heads, 2)), sem((heads, 2)), sem((heads, 2)),
            sem((num_chips * CORES,)), sem((num_chips * CORES,)),
        ],
        compiler_params=pltpu.CompilerParams(vmem_limit_bytes=60 * 2 ** 20, collective_id=0, has_side_effects=True),
        cost_estimate=pl.CostEstimate(flops=50_000_000_000, bytes_accessed=64_000_000, transcendentals=40_000_000),
        name='attn_grads',
    )(q, d_out, stats, kv, k_raw, cos_q, sin_q, cos_k, sin_k, wq, wk)


def solution(mesh):
    cp_size = mesh.shape['cp']
    num_chips = cp_size // CORES

    def local_grads(q_raw, k_raw, v_proj, out_fwd, lse_fwd, d_out, q_norm, k_norm):
        dev_rank = lax.axis_index('cp')
        chip = dev_rank // CORES
        local_rows, num_heads = q_raw.shape[0], q_raw.shape[1]
        chunk_len = local_rows // 2
        kv_heads = k_raw.shape[1]
        per_kv = num_heads // kv_heads

        num_chunks = 2 * cp_size
        offsets = jnp.arange(chunk_len)
        chip_chunks = jnp.stack([2 * chip, 2 * chip + 1, num_chunks - 2 - 2 * chip, num_chunks - 1 - 2 * chip])
        cos_q, sin_q = rope_tables(chip_chunks[:, None] * chunk_len + offsets)
        dev_chunks = jnp.stack([dev_rank, num_chunks - 1 - dev_rank])
        cos_k, sin_k = rope_tables(dev_chunks[:, None] * chunk_len + offsets)

        q_h, do_h, stats, kv, k_h = prepare(q_raw, d_out, out_fwd, k_raw, v_proj, lse_fwd, cos_k, sin_k, k_norm[None])
        stacked = (kv_heads, 2, per_kv * chunk_len, HEAD_DIM)
        cos_qt, sin_qt = jnp.swapaxes(cos_q, 1, 2), jnp.swapaxes(sin_q, 1, 2)
        wq_t = jnp.broadcast_to(q_norm[:, None], (HEAD_DIM, chunk_len))
        dq, dk, dv, weights = attn_grads(num_chips, q_h.reshape(stacked), do_h.reshape(stacked), stats, kv, k_h,
                                         cos_qt, sin_qt, cos_k, sin_k, wq_t, k_norm[None])
        dq_raw, dk_raw, dv_home = finish(dq.reshape(q_h.shape), dk, dv)
        return dq_raw, dk_raw, dv_home, weights[0], weights[1]

    row_spec = P(('dp', 'cp'))
    in_specs = (row_spec, row_spec, row_spec, row_spec, row_spec, row_spec, P(), P())
    out_specs = (row_spec, row_spec, row_spec, P('dp'), P('dp'))
    return jax.shard_map(local_grads, mesh=mesh, in_specs=in_specs, out_specs=out_specs, check_vma=False)
```

```python
import functools

import jax
import jax.numpy as jnp
from jax import lax
from jax.experimental import pallas as pl
from jax.experimental.pallas import tpu as pltpu
from jax.sharding import PartitionSpec as P

HEAD_DIM = 128
ROPE_THETA = 1000000.0
NORM_EPS = 1e-6
LOG2E = 1.4426950408889634
SM_SCALE = HEAD_DIM ** -0.5
CORES = 2
MESH = pl.DeviceIdType.MESH


def rope_tables(positions):
    inv_freq = ROPE_THETA ** (-jnp.arange(0, HEAD_DIM, 2).astype(jnp.float32) / HEAD_DIM)
    angles = positions.astype(jnp.float32)[..., None] * inv_freq
    cos_t, sin_t = jnp.cos(angles), jnp.sin(angles)
    return jnp.concatenate([cos_t, cos_t], axis=-1), jnp.concatenate([-sin_t, sin_t], axis=-1)


def swap_halves(arr):
    return pltpu.roll(arr, HEAD_DIM // 2, arr.ndim - 1)


def inverse_rms(raw_in):
    return lax.rsqrt(jnp.mean(raw_in * raw_in, axis=-1, keepdims=True) + NORM_EPS)


def norm_rope_pull(raw_in, weight, cos_t, sin_t, grad):
    inv_rms = inverse_rms(raw_in)
    unit = raw_in * inv_rms
    grad_normed = grad * cos_t - swap_halves(grad) * sin_t
    weight_terms = grad_normed * unit
    grad_unit = grad_normed * weight
    grad_raw = inv_rms * (grad_unit - unit * jnp.mean(grad_unit * unit, axis=-1, keepdims=True))
    return grad_raw, weight_terms.reshape(-1, 8, HEAD_DIM).sum(0)


def swap_rows(arr):
    return jnp.concatenate([arr[HEAD_DIM // 2:], arr[:HEAD_DIM // 2]], axis=0)


def inverse_rms_t(raw_in):
    return lax.rsqrt(jnp.mean(raw_in * raw_in, axis=0, keepdims=True) + NORM_EPS)


def dot(a, b):
    return lax.dot_general(a, b, (((1,), (0,)), ((), ())), preferred_element_type=jnp.float32)


def attn_kernel(num_chips, q_hbm, do_hbm, st_hbm, kv_hbm, k_hbm, tables_hbm, k_tables_hbm, wq_row, wk,
                dq_hbm, dkv_hbm, dw_out,
                k_raw, tables, k_tables, wq, dkv_out,
                q_buf, do_buf, st_buf, kv_buf, raw_now, q_now, qt_now, dot_now, dqt_now, kt_now, p_now, ds_now,
                acc, own_acc, own_recv, send_buf, transit, part, total, dwq_acc, dw_acc, dw_all,
                ex_send, ex_recv, ex_local, own_send, own_kv_recv, own_local, nb_send, nb_recv, rl_send, op_recv,
                pt_send, pt_recv, tr_send, tr_recv, fw_send, fw_recv, oa_send, oa_recv,
                dq_send, dq_recv, dq_local, dw_send, dw_recv, in_local, out_local):
    me = lax.axis_index('cp')
    chip, core = me // CORES, me % CORES
    left, right = (chip + num_chips - 1) % num_chips, (chip + 1) % num_chips
    far = (chip + 2) % num_chips
    heads = q_buf.shape[0]
    num_chunks, chunk_len = kv_buf.shape[2], kv_buf.shape[4]
    per_kv = q_buf.shape[2] // chunk_len
    cos_q, sin_q = tables.at[0], tables.at[1]
    cos_k, sin_k = k_tables.at[0], k_tables.at[1]

    def in_copy(i):
        src, dst = ((tables_hbm, tables), (k_tables_hbm, k_tables), (k_hbm, k_raw))[i]
        return pltpu.make_async_copy(src, dst, in_local.at[i])

    def out_copy(head):
        return pltpu.make_async_copy(dkv_out.at[head], dkv_hbm.at[head], out_local.at[head])

    def remote(src, dst, send_sem, recv_sem, to_chip, to_core):
        return pltpu.make_async_remote_copy(src_ref=src, dst_ref=dst, send_sem=send_sem, recv_sem=recv_sem,
                                            device_id={'cp': to_chip * CORES + to_core}, device_id_type=MESH)

    def place(of_core, ch):
        return of_core if ch == 0 else num_chunks - 1 - of_core

    exchanged = ((q_hbm, q_buf), (do_hbm, do_buf), (st_hbm, st_buf))

    def ex_copies(h):
        for a, (src, dst) in enumerate(exchanged):
            for ch in range(2):
                mine = place(core, ch)
                yield (remote(src.at[(1 - core) * heads + h, ch], dst.at[h, mine], ex_send.at[h, a, ch], ex_recv.at[h, a, ch], chip, 1 - core),
                       remote(src.at[(1 - core) * heads + h, ch], dst.at[h, place(1 - core, ch)], ex_send.at[h, a, ch], ex_recv.at[h, a, ch], chip, 1 - core),
                       pltpu.make_async_copy(src.at[core * heads + h, ch], dst.at[h, mine], ex_local.at[h, a, ch]))

    def own_copies(h):
        for ch in range(2):
            mine = place(core, ch)
            yield (remote(kv_hbm.at[(1 - core) * heads + h, ch], kv_buf.at[0, h, mine], own_send.at[h, ch], own_kv_recv.at[h, ch], chip, 1 - core),
                   remote(kv_hbm.at[(1 - core) * heads + h, ch], kv_buf.at[0, h, place(1 - core, ch)], own_send.at[h, ch], own_kv_recv.at[h, ch], chip, 1 - core),
                   pltpu.make_async_copy(kv_hbm.at[core * heads + h, ch], kv_buf.at[0, h, mine], own_local.at[h, ch]))

    def nb_out(h, to_core, ch, way):
        return remote(kv_hbm.at[to_core * heads + h, ch], kv_buf.at[3 if way == 0 else 1, h, place(core, ch)],
                      nb_send.at[h, to_core, ch, way], nb_recv.at[h, place(core, ch), way], right if way == 0 else left, to_core)

    def second_sent(way):
        return chip >= 2 if way == 0 else chip >= 1

    def nb_each(h, fn):
        for way in range(2):
            for to_core in range(CORES):
                fn(nb_out(h, to_core, 0, way))

            @pl.when(second_sent(way))
            def _():
                for to_core in range(CORES):
                    fn(nb_out(h, to_core, 1, way))

    def nb_wait(h, way):
        slot = 3 if way == 0 else 1

        def wait(idx):
            remote(kv_hbm.at[0, 0], kv_buf.at[slot, h, idx], nb_send.at[h, 0, 0, way], nb_recv.at[h, idx, way], left, core).wait_recv()

        wait(0)
        wait(1)

        @pl.when(left >= 2 if way == 0 else right >= 1)
        def _():
            wait(2)
            wait(3)

    def relay(h, second, kind):
        src_slot, to_chip = (3, right) if kind == 0 else (1, left)
        pair = pl.ds(2 * second, 2)
        return remote(kv_buf.at[src_slot, h, pair, kind], kv_buf.at[2, h, pair, kind], rl_send.at[h, second, kind], op_recv.at[h, second, kind], to_chip, core)

    def relay_each(h, fn):
        for kind in range(2):
            fn(relay(h, 0, kind))

            @pl.when(right < left if kind == 0 else left < right)
            def _():
                fn(relay(h, 1, kind))

    def part_out(h, off, idx):
        to_chip = right if off == 1 else left
        home_core = idx if idx < 2 else num_chunks - 1 - idx
        return remote(send_buf.at[h, off - 1, idx], part.at[2 if off == 1 else 0, core * heads + h, idx // 2],
                      pt_send.at[h, off // 2, idx], pt_recv.at[1 if off == 1 else 0, core * heads + h, idx // 2], to_chip, home_core)

    def transit_out(h, second, kind):
        pair = pl.ds(2 * second, 2)
        return remote(send_buf.at[h, 1, pair, kind], transit.at[h, kind, pair], tr_send.at[h, second, kind], tr_recv.at[h, second, kind],
                      right if kind == 0 else left, core)

    def forward_out(h, idx, kind):
        home_core = idx if idx < 2 else num_chunks - 1 - idx
        return remote(transit.at[h, kind, idx], part.at[1, core * heads + h, idx // 2, kind],
                      fw_send.at[h, idx, kind], fw_recv.at[core * heads + h, idx // 2, kind], right if kind == 0 else left, home_core)

    def forward_each(h, fn):
        for kind in range(2):
            fn(h, 0, kind)

            @pl.when(left < right if kind == 0 else right < left)
            def _():
                fn(h, 1, kind)

    def start_forward(h, second, kind):
        transit_out(h, second, kind).wait_recv()
        for idx in (2 * second, 2 * second + 1):
            forward_out(h, idx, kind).start()

    def end_forward(h, second, kind):
        for idx in (2 * second, 2 * second + 1):
            forward_out(h, idx, kind).wait_send()

    def own_out(h, ch):
        return remote(own_acc.at[h, place(1 - core, ch)], own_recv.at[h, ch], oa_send.at[h, ch], oa_recv.at[h, ch], chip, 1 - core)

    def dq_copies(h):
        for ch in range(2):
            yield (remote(q_buf.at[h, place(1 - core, ch)], dq_hbm.at[core * heads + h, ch], dq_send.at[h, ch], dq_recv.at[h, ch], chip, 1 - core),
                   remote(q_buf.at[h, place(1 - core, ch)], dq_hbm.at[(1 - core) * heads + h, ch], dq_send.at[h, ch], dq_recv.at[h, ch], chip, 1 - core),
                   pltpu.make_async_copy(q_buf.at[h, place(core, ch)], dq_hbm.at[core * heads + h, ch], dq_local.at[h, ch]))

    def dw_out_to(step):
        peer = (me + step) % (num_chips * CORES)
        return remote(dw_acc, dw_all.at[me], dw_send.at[step], dw_recv.at[me], peer // CORES, peer % CORES)

    def block(h, off, kc, qb, masked, slot=0):
        k_blk, v_blk = kv_buf[off, h, kc, 0], kv_buf[off, h, kc, 1]
        if masked:
            key_pos = lax.broadcasted_iota(jnp.int32, (chunk_len, chunk_len), 0)
            query_pos = lax.broadcasted_iota(jnp.int32, (chunk_len, chunk_len), 1)
            visible = key_pos <= query_pos
        for g in range(per_kv):
            cols = pl.ds(g * chunk_len, chunk_len)
            logits = dot(k_blk, qt_now[qb, :, cols]) * (SM_SCALE * LOG2E) - st_buf[h, qb, 0, g:g + 1, :]
            if masked:
                logits = jnp.where(visible, logits, -jnp.inf)
            prob = jnp.exp2(logits)
            dprob = dot(v_blk, dot_now[qb, :, cols])
            p_now[slot, :, cols] = prob.astype(jnp.bfloat16)
            ds_now[slot, :, cols] = (prob * (dprob - st_buf[h, qb, 1, g:g + 1, :])).astype(jnp.bfloat16)
        acc[kc, 1] += dot(p_now[slot], do_buf[h, qb])
        acc[kc, 0] += dot(ds_now[slot], q_now[qb])
        dqt_now[qb] += dot(kt_now[...], ds_now[slot])

    def source_block(h, off):
        src = (chip + off) % num_chips
        own = off == 0
        early = src < chip
        acc[...] = jnp.zeros_like(acc)

        @pl.loop(0, jnp.where(early, num_chunks // 2, num_chunks))
        def _(kc):
            kt_now[...] = kv_buf[off, h, kc, 0].T

            @pl.when(own)
            def _():
                block(h, off, kc, kc, True)

                @pl.loop(kc + 1, num_chunks)
                def _(qb):
                    block(h, off, kc, qb, False)

            @pl.when(jnp.logical_not(own))
            def _():
                @pl.loop(jnp.where(early, 0, num_chunks // 4), num_chunks // 2)
                def _(pair):
                    block(h, off, kc, 2 * pair, False)
                    block(h, off, kc, 2 * pair + 1, False, 1)

    def home(head, h, own):
        for ch in range(2):
            mine = place(core, ch)
            total[...] = own_acc[h, mine] if own else own_recv[h, ch]

            def add(slot):
                total[...] += part[slot, head, ch].astype(jnp.float32)

            def take_side(way):
                remote(send_buf.at[0, 0, 0], part.at[2 * way, head, ch], pt_send.at[0, 0, 0], pt_recv.at[way, head, ch], left, core).wait_recv()
                add(2 * way)

            def take_far():
                for kind in range(2):
                    remote(transit.at[0, 0, 0], part.at[1, head, ch, kind], fw_send.at[0, 0, 0], fw_recv.at[head, ch, kind], left, core).wait_recv()
                add(1)

            if ch == 0:
                take_side(0)
                take_side(1)
                take_far()
            else:
                @pl.when(right < chip)
                def _():
                    take_side(0)

                @pl.when(left < chip)
                def _():
                    take_side(1)

                @pl.when(far < chip)
                def _():
                    take_far()

            raw = k_raw[head, ch].astype(jnp.float32)
            grad_raw, terms = norm_rope_pull(raw, wk[...], cos_k[ch], sin_k[ch], total[0] * SM_SCALE)
            dkv_out[head, 0, ch] = grad_raw.astype(jnp.bfloat16)
            dkv_out[head, 1, ch] = total[1].astype(jnp.bfloat16)
            dw_acc[1] += terms
        out_copy(head).start()

    def home_head(h):
        for ch in range(2):
            own_out(h, ch).wait_recv()
            own_out(h, ch).wait_send()
        home((1 - core) * heads + h, h, False)
        home(core * heads + h, h, True)

    def compute_head(h):
        for copies in (own_copies(h), ex_copies(h)):
            for out, arriving, local in copies:
                out.wait_send()
                arriving.wait_recv()
                local.wait()
        dqt_now[...] = jnp.zeros_like(dqt_now)

        @pl.loop(0, num_chunks)
        def _(qb):
            for g in range(per_kv):
                rows = pl.ds(g * chunk_len, chunk_len)
                raw_bf = q_buf[h, qb, rows, :].T
                raw_now[qb, :, rows] = raw_bf
                raw = raw_bf.astype(jnp.float32)
                normed = raw * inverse_rms_t(raw) * wq[...]
                query = (normed * cos_q[qb] + swap_rows(normed) * sin_q[qb]).astype(jnp.bfloat16)
                qt_now[qb, :, rows] = query
                q_now[qb, rows, :] = query.T
            dot_now[qb] = do_buf[h, qb].T

        last = h == heads - 1

        @pl.loop(0, num_chips)
        def _(j):
            orders = [sum(off * 4 ** i for i, off in enumerate(order)) for order in ((0, 3, 1, 2), (0, 1, 3, 2), (3, 1, 0, 2), (2, 1, 3, 0))]
            order = jnp.where(h == 0, orders[0], jnp.where(last, orders[3], jnp.where(h == 1, orders[1], orders[2])))
            off = order // jnp.where(j == 0, 1, jnp.where(j == 1, 4, jnp.where(j == 2, 16, 64))) % 4

            @pl.when(off == 2)
            def _():
                for kind in range(2):
                    relay(h, 0, kind).wait_recv()

                @pl.when(chip < far)
                def _():
                    for kind in range(2):
                        relay(h, 1, kind).wait_recv()

            source_block(h, off)
            src = (chip + off) % num_chips

            @pl.when(off == 0)
            def _():
                own_acc[h] = acc[...]
                for ch in range(2):
                    own_out(h, ch).start()

            @pl.when(off != 0)
            def _():
                send_buf[h, off - 1, 0:2] = acc[0:2].astype(jnp.bfloat16)

                @pl.when(chip < src)
                def _():
                    send_buf[h, off - 1, 2:4] = acc[2:4].astype(jnp.bfloat16)

            for side in (1, 3):
                @pl.when(off == side)
                def _():
                    part_out(h, side, 0).start()
                    part_out(h, side, 1).start()

                    @pl.when(chip < src)
                    def _():
                        part_out(h, side, 2).start()
                        part_out(h, side, 3).start()

            @pl.when(off == 2)
            def _():
                for kind in range(2):
                    transit_out(h, 0, kind).start()

                @pl.when(chip < src)
                def _():
                    for kind in range(2):
                        transit_out(h, 1, kind).start()

            def pass_keys(of_head):
                nb_wait(of_head, 0)
                nb_wait(of_head, 1)
                relay_each(of_head, lambda copy: copy.start())

            @pl.when((h == 0) & (j == 0))
            def _():
                pass_keys(0)

            @pl.when((h + 1 < heads) & (j == jnp.where(h == 0, 2, 0)))
            def _():
                pass_keys(h + 1)

            @pl.when((h + 2 < heads) & (j == jnp.where(h == 0, 1, 0)))
            def _():
                nb_each(h + 2, lambda copy: copy.start())

            @pl.when((h > 0) & (j == jnp.where(last, 0, 2)))
            def _():
                forward_each(h - 1, start_forward)

            @pl.when(last & (j == 1))
            def _():
                forward_each(h, start_forward)

        @pl.loop(0, num_chunks)
        def _(qb):
            for g in range(per_kv):
                rows = pl.ds(g * chunk_len, chunk_len)
                grad = dqt_now[qb, :, rows] * SM_SCALE
                raw = raw_now[qb, :, rows].astype(jnp.float32)
                inv_rms = inverse_rms_t(raw)
                unit = raw * inv_rms
                grad_normed = grad * cos_q[qb] - swap_rows(grad) * sin_q[qb]
                dwq_acc[...] += grad_normed * unit
                grad_unit = grad_normed * wq[...]
                grad_raw = inv_rms * (grad_unit - unit * jnp.mean(grad_unit * unit, axis=0, keepdims=True))
                q_buf[h, qb, rows, :] = grad_raw.astype(jnp.bfloat16).T

        for out, _, local in dq_copies(h):
            out.start()
            local.start()

    barrier = pltpu.get_barrier_semaphore()
    for step in range(1, num_chips * CORES):
        pl.semaphore_signal(barrier, inc=1, device_id={'cp': (me + step) % (num_chips * CORES)}, device_id_type=MESH)
    pl.semaphore_wait(barrier, num_chips * CORES - 1)

    nb_each(0, lambda copy: copy.start())
    in_copy(0).start()

    @pl.loop(0, heads)
    def _(h):
        for out, _, local in own_copies(h):
            out.start()
            local.start()
        for out, _, local in ex_copies(h):
            out.start()
            local.start()

    nb_each(1, lambda copy: copy.start())
    in_copy(1).start()
    in_copy(2).start()
    wq[...] = jnp.broadcast_to(wq_row[...], (chunk_len, HEAD_DIM)).T
    in_copy(0).wait()
    in_copy(1).wait()
    in_copy(2).wait()
    dw_acc[...] = jnp.zeros_like(dw_acc)
    dwq_acc[...] = jnp.zeros_like(dwq_acc)

    @pl.loop(0, heads + 3)
    def _(h):
        @pl.when(h < heads)
        def _():
            compute_head(h)

        @pl.when(h >= 3)
        def _():
            home_head(h - 3)

    dw_acc[0] = dwq_acc[...].T.reshape(-1, 8, HEAD_DIM).sum(0)
    for step in range(1, num_chips * CORES):
        dw_out_to(step).start()
    dw_all[me] = dw_acc[...]

    @pl.loop(0, heads)
    def _(h):
        nb_each(h, lambda copy: copy.wait_send())
        relay_each(h, lambda copy: copy.wait_send())
        for off in (1, 3):
            part_out(h, off, 0).wait_send()
            part_out(h, off, 1).wait_send()

            @pl.when(chip < (chip + off) % num_chips)
            def _():
                part_out(h, off, 2).wait_send()
                part_out(h, off, 3).wait_send()
        for kind in range(2):
            transit_out(h, 0, kind).wait_send()

        @pl.when(chip < far)
        def _():
            for kind in range(2):
                transit_out(h, 1, kind).wait_send()
        forward_each(h, end_forward)
        for out, arriving, local in dq_copies(h):
            out.wait_send()
            arriving.wait_recv()
            local.wait()
        out_copy(h).wait()
        out_copy(heads + h).wait()

    for step in range(1, num_chips * CORES):
        peer = (me + step) % (num_chips * CORES)
        dw_out_to(step).wait_send()
        remote(dw_acc, dw_all.at[peer], dw_send.at[step], dw_recv.at[peer], chip, core).wait_recv()
    dw_out[...] = dw_all[...].sum(0).sum(1)


def prepare_kernel(q_ref, do_ref, out_ref, k_ref, v_ref, lse_ref, k_table, wk, q_out, do_out, st_out, kv_out, k_out):
    rows, num_heads = q_ref.shape[0], q_ref.shape[1]
    kv_heads = k_ref.shape[1]
    f32, bf16 = jnp.float32, jnp.bfloat16

    def by_head(arr):
        return jnp.swapaxes(arr, 0, 1)

    d_out = do_ref[...].astype(f32)
    q_out[:, 0] = by_head(q_ref[...].astype(f32)).astype(bf16).reshape(kv_heads, -1, rows, HEAD_DIM)
    do_out[:, 0] = by_head(d_out).astype(bf16).reshape(kv_heads, -1, rows, HEAD_DIM)
    delta = jnp.sum(d_out * out_ref[...].astype(f32), axis=-1)
    st_out[:, 0, 0] = (lse_ref[...] * LOG2E).reshape(kv_heads, -1, rows)
    st_out[:, 0, 1] = delta.T.reshape(kv_heads, -1, rows)
    raw = k_ref[...].astype(f32)
    normed = raw * inverse_rms(raw) * wk[...]
    key = normed * k_table[0, 0][:, None] + swap_halves(normed) * k_table[1, 0][:, None]
    kv_out[:, 0, 0] = by_head(key).astype(bf16)
    kv_out[:, 0, 1] = by_head(v_ref[...].astype(f32)).astype(bf16)
    k_out[:, 0] = by_head(raw).astype(bf16)


def prepare(q_raw, d_out, out_fwd, k_raw, v_proj, lse_t, k_tables, wk, rows=128):
    local_rows, num_heads, _ = q_raw.shape
    kv_heads = k_raw.shape[1]
    per_kv, chunk_len = num_heads // kv_heads, local_rows // 2
    parts = chunk_len // rows
    bf16 = jnp.bfloat16
    rows_q = pl.BlockSpec((rows, num_heads, HEAD_DIM), lambda i: (i, 0, 0))
    rows_k = pl.BlockSpec((rows, kv_heads, HEAD_DIM), lambda i: (i, 0, 0))
    table = pl.BlockSpec((2, 1, rows, HEAD_DIM), lambda i: (0, i // parts, i % parts, 0))
    heads_q = pl.BlockSpec((kv_heads, 1, per_kv, rows, HEAD_DIM), lambda i: (0, i // parts, 0, i % parts, 0))
    return pl.pallas_call(
        prepare_kernel,
        grid=(2 * parts,),
        in_specs=[rows_q, rows_q, rows_q, rows_k, rows_k, pl.BlockSpec((num_heads, rows), lambda i: (0, i)), table,
                  pl.BlockSpec((1, HEAD_DIM), lambda i: (0, 0))],
        out_specs=[heads_q, heads_q,
                   pl.BlockSpec((kv_heads, 1, 2, per_kv, rows), lambda i: (0, i // parts, 0, 0, i % parts)),
                   pl.BlockSpec((kv_heads, 1, 2, rows, HEAD_DIM), lambda i: (0, i // parts, 0, i % parts, 0)),
                   pl.BlockSpec((kv_heads, 1, rows, HEAD_DIM), lambda i: (0, i // parts, i % parts, 0))],
        out_shape=[jax.ShapeDtypeStruct((kv_heads, 2, per_kv, chunk_len, HEAD_DIM), bf16),
                   jax.ShapeDtypeStruct((kv_heads, 2, per_kv, chunk_len, HEAD_DIM), bf16),
                   jax.ShapeDtypeStruct((kv_heads, 2, 2, per_kv, chunk_len), jnp.float32),
                   jax.ShapeDtypeStruct((kv_heads, 2, 2, chunk_len, HEAD_DIM), bf16),
                   jax.ShapeDtypeStruct((kv_heads, 2, chunk_len, HEAD_DIM), bf16)],
        compiler_params=pltpu.CompilerParams(vmem_limit_bytes=48 * 2 ** 20),
        name='prepare',
    )(q_raw, d_out, out_fwd, k_raw, v_proj, lse_t, k_tables, wk)


def finish_kernel(dq_ref, dkv_ref, dq_out, dk_out, dv_out):
    for src, dst in ((dq_ref, dq_out), (dkv_ref.at[:, 0], dk_out), (dkv_ref.at[:, 1], dv_out)):
        by_head = src[:, 0].reshape(-1, src.shape[-2], HEAD_DIM).astype(jnp.float32)
        dst[...] = jnp.swapaxes(by_head, 0, 1).astype(jnp.bfloat16)


def finish(dq, dkv, rows=128):
    kv_heads, _, per_kv, chunk_len, _ = dq.shape
    parts = chunk_len // rows
    num_heads = kv_heads * per_kv
    heads_k = pl.BlockSpec((kv_heads, 2, 1, rows, HEAD_DIM), lambda i: (0, 0, i // parts, i % parts, 0))
    rows_k = pl.BlockSpec((rows, kv_heads, HEAD_DIM), lambda i: (i, 0, 0))
    out_k = jax.ShapeDtypeStruct((2 * chunk_len, kv_heads, HEAD_DIM), jnp.bfloat16)
    return pl.pallas_call(
        finish_kernel,
        grid=(2 * parts,),
        in_specs=[pl.BlockSpec((kv_heads, 1, per_kv, rows, HEAD_DIM), lambda i: (0, i // parts, 0, i % parts, 0)), heads_k],
        out_specs=[pl.BlockSpec((rows, num_heads, HEAD_DIM), lambda i: (i, 0, 0)), rows_k, rows_k],
        out_shape=[jax.ShapeDtypeStruct((2 * chunk_len, num_heads, HEAD_DIM), jnp.bfloat16), out_k, out_k],
        compiler_params=pltpu.CompilerParams(vmem_limit_bytes=48 * 2 ** 20),
        name='finish',
    )(dq, dkv)


def attn_grads(num_chips, q, d_out, stats, kv, k_raw, tables, k_tables, wq, wk):
    kv_heads, _, rows, _ = q.shape
    chunk_len = kv.shape[3]
    heads = kv_heads // CORES
    half = (2, chunk_len, HEAD_DIM)
    bf16, f32 = jnp.bfloat16, jnp.float32
    sem = pltpu.SemaphoreType.DMA
    any_spec, vmem = pl.BlockSpec(memory_space=pl.ANY), pl.BlockSpec(memory_space=pltpu.VMEM)
    return pl.pallas_call(
        functools.partial(attn_kernel, num_chips),
        in_specs=[any_spec] * 7 + [vmem] * 2,
        out_specs=[any_spec, any_spec, vmem],
        out_shape=[jax.ShapeDtypeStruct(q.shape, bf16), jax.ShapeDtypeStruct((kv_heads, 2) + k_raw.shape[1:], bf16),
                   jax.ShapeDtypeStruct((2, HEAD_DIM), f32)],
        scratch_shapes=[
            pltpu.VMEM(k_raw.shape, bf16),
            pltpu.VMEM(tables.shape, f32),
            pltpu.VMEM(k_tables.shape, f32),
            pltpu.VMEM((HEAD_DIM, chunk_len), f32),
            pltpu.VMEM((kv_heads, 2) + k_raw.shape[1:], bf16),
            pltpu.VMEM((heads, 4, rows, HEAD_DIM), bf16),
            pltpu.VMEM((heads, 4, rows, HEAD_DIM), bf16),
            pltpu.VMEM((heads, 4) + stats.shape[2:], f32),
            pltpu.VMEM((num_chips, heads, 4) + half, bf16),
            pltpu.VMEM((4, HEAD_DIM, rows), bf16),
            pltpu.VMEM((4, rows, HEAD_DIM), bf16),
            pltpu.VMEM((4, HEAD_DIM, rows), bf16),
            pltpu.VMEM((4, HEAD_DIM, rows), bf16),
            pltpu.VMEM((4, HEAD_DIM, rows), f32),
            pltpu.VMEM((HEAD_DIM, chunk_len), bf16),
            pltpu.VMEM((2, chunk_len, rows), bf16),
            pltpu.VMEM((2, chunk_len, rows), bf16),
            pltpu.VMEM((4,) + half, f32),
            pltpu.VMEM((heads, 4) + half, f32),
            pltpu.VMEM((heads, 2) + half, f32),
            pltpu.VMEM((heads, 3, 4) + half, bf16),
            pltpu.VMEM((heads, 2, 4, chunk_len, HEAD_DIM), bf16),
            pltpu.VMEM((3, kv_heads, 2) + half, bf16),
            pltpu.VMEM(half, f32),
            pltpu.VMEM((HEAD_DIM, chunk_len), f32),
            pltpu.VMEM((2, 8, HEAD_DIM), f32),
            pltpu.VMEM((num_chips * CORES, 2, 8, HEAD_DIM), f32),
            sem((heads, 3, 2)), sem((heads, 3, 2)), sem((heads, 3, 2)),
            sem((heads, 2)), sem((heads, 2)), sem((heads, 2)),
            sem((heads, CORES, 2, 2)), sem((heads, 4, 2)),
            sem((heads, 2, 2)), sem((heads, 2, 2)),
            sem((heads, 2, 4)), sem((2, kv_heads, 2)),
            sem((heads, 2, 2)), sem((heads, 2, 2)),
            sem((heads, 4, 2)), sem((kv_heads, 2, 2)),
            sem((heads, 2)), sem((heads, 2)),
            sem((heads, 2)), sem((heads, 2)), sem((heads, 2)),
            sem((num_chips * CORES,)), sem((num_chips * CORES,)),
            sem((3,)), sem((kv_heads,)),
        ],
        compiler_params=pltpu.CompilerParams(vmem_limit_bytes=60 * 2 ** 20, collective_id=0, has_side_effects=True),
        cost_estimate=pl.CostEstimate(flops=50_000_000_000, bytes_accessed=64_000_000, transcendentals=40_000_000),
        name='attn_grads',
    )(q, d_out, stats, kv, k_raw, tables, k_tables, wq, wk)


def solution(mesh):
    cp_size = mesh.shape['cp']
    num_chips = cp_size // CORES

    def local_grads(q_raw, k_raw, v_proj, out_fwd, lse_fwd, d_out, q_norm, k_norm):
        dev_rank = lax.axis_index('cp')
        chip = dev_rank // CORES
        local_rows, num_heads = q_raw.shape[0], q_raw.shape[1]
        chunk_len = local_rows // 2
        kv_heads = k_raw.shape[1]
        per_kv = num_heads // kv_heads

        num_chunks = 2 * cp_size
        offsets = jnp.arange(chunk_len)
        chip_chunks = jnp.stack([2 * chip, 2 * chip + 1, num_chunks - 2 - 2 * chip, num_chunks - 1 - 2 * chip])
        inv_freq = ROPE_THETA ** (-jnp.arange(0, HEAD_DIM, 2).astype(jnp.float32) / HEAD_DIM)
        angles = inv_freq[None, :, None] * (chip_chunks[:, None] * chunk_len + offsets).astype(jnp.float32)[:, None, :]
        cos_t, sin_t = jnp.cos(angles), jnp.sin(angles)
        tables = jnp.stack([jnp.concatenate([cos_t, cos_t], axis=1), jnp.concatenate([-sin_t, sin_t], axis=1)])
        dev_chunks = jnp.stack([dev_rank, num_chunks - 1 - dev_rank])
        k_tables = jnp.stack(rope_tables(dev_chunks[:, None] * chunk_len + offsets))

        q_h, do_h, stats, kv, k_h = prepare(q_raw, d_out, out_fwd, k_raw, v_proj, lse_fwd.T, k_tables, k_norm[None])
        stacked = (kv_heads, 2, per_kv * chunk_len, HEAD_DIM)
        dq, dkv, weights = attn_grads(num_chips, q_h.reshape(stacked), do_h.reshape(stacked), stats, kv, k_h,
                                      tables, k_tables, q_norm[None], k_norm[None])
        dq_raw, dk_raw, dv_home = finish(dq.reshape(q_h.shape), dkv)
        return dq_raw, dk_raw, dv_home, weights[0], weights[1]

    row_spec = P(('dp', 'cp'))
    in_specs = (row_spec, row_spec, row_spec, row_spec, row_spec, row_spec, P(), P())
    out_specs = (row_spec, row_spec, row_spec, P('dp'), P('dp'))
    return jax.shard_map(local_grads, mesh=mesh, in_specs=in_specs, out_specs=out_specs, check_vma=False)
```

```python
import functools

import jax
import jax.numpy as jnp
from jax import lax
from jax.experimental import pallas as pl
from jax.experimental.pallas import tpu as pltpu
from jax.sharding import PartitionSpec as P

HEAD_DIM = 128
ROPE_THETA = 1000000.0
NORM_EPS = 1e-6
LOG2E = 1.4426950408889634
SM_SCALE = HEAD_DIM ** -0.5
CORES = 2
MESH = pl.DeviceIdType.MESH


def rope_tables(positions):
    inv_freq = ROPE_THETA ** (-jnp.arange(0, HEAD_DIM, 2).astype(jnp.float32) / HEAD_DIM)
    angles = positions.astype(jnp.float32)[..., None] * inv_freq
    cos_t, sin_t = jnp.cos(angles), jnp.sin(angles)
    return jnp.concatenate([cos_t, cos_t], axis=-1), jnp.concatenate([-sin_t, sin_t], axis=-1)


def swap_halves(arr):
    return pltpu.roll(arr, HEAD_DIM // 2, arr.ndim - 1)


def inverse_rms(raw_in):
    return lax.rsqrt(jnp.mean(raw_in * raw_in, axis=-1, keepdims=True) + NORM_EPS)


def norm_rope_pull(raw_in, weight, cos_t, sin_t, grad):
    inv_rms = inverse_rms(raw_in)
    unit = raw_in * inv_rms
    grad_normed = grad * cos_t - swap_halves(grad) * sin_t
    weight_terms = grad_normed * unit
    grad_unit = grad_normed * weight
    grad_raw = inv_rms * (grad_unit - unit * jnp.mean(grad_unit * unit, axis=-1, keepdims=True))
    return grad_raw, weight_terms.reshape(-1, 8, HEAD_DIM).sum(0)


def swap_rows(arr):
    return jnp.concatenate([arr[HEAD_DIM // 2:], arr[:HEAD_DIM // 2]], axis=0)


def inverse_rms_t(raw_in):
    return lax.rsqrt(jnp.mean(raw_in * raw_in, axis=0, keepdims=True) + NORM_EPS)


def dot(a, b):
    return lax.dot_general(a, b, (((1,), (0,)), ((), ())), preferred_element_type=jnp.float32)


def attn_kernel(num_chips, q_hbm, do_hbm, st_hbm, kv_hbm, k_hbm, tables_hbm, k_tables_hbm, wq_row, wk,
                dq_hbm, dkv_hbm, dw_out,
                k_raw, tables, k_tables, wq, dkv_out,
                q_buf, do_buf, st_buf, kv_buf, raw_now, q_now, qt_now, dot_now, dqt_now, kt_now, p_now, ds_now,
                acc, own_acc, own_recv, send_buf, transit, part, total, dwq_acc, dw_acc, dw_all,
                ex_send, ex_recv, ex_local, own_send, own_kv_recv, own_local, nb_send, nb_recv, rl_send, op_recv,
                pt_send, pt_recv, tr_send, tr_recv, fw_send, fw_recv, oa_send, oa_recv,
                dq_send, dq_recv, dq_local, dw_send, dw_recv, in_local, out_local):
    me = lax.axis_index('cp')
    chip, core = me // CORES, me % CORES
    left, right = (chip + num_chips - 1) % num_chips, (chip + 1) % num_chips
    far = (chip + 2) % num_chips
    heads = q_buf.shape[0]
    num_chunks, chunk_len = kv_buf.shape[2], kv_buf.shape[4]
    per_kv = q_buf.shape[2] // chunk_len
    cos_q, sin_q = tables.at[0], tables.at[1]
    cos_k, sin_k = k_tables.at[0], k_tables.at[1]

    def in_copy(i):
        src, dst = ((tables_hbm, tables), (k_tables_hbm, k_tables), (k_hbm, k_raw))[i]
        return pltpu.make_async_copy(src, dst, in_local.at[i])

    def out_copy(head):
        return pltpu.make_async_copy(dkv_out.at[head], dkv_hbm.at[head], out_local.at[head])

    def remote(src, dst, send_sem, recv_sem, to_chip, to_core):
        return pltpu.make_async_remote_copy(src_ref=src, dst_ref=dst, send_sem=send_sem, recv_sem=recv_sem,
                                            device_id={'cp': to_chip * CORES + to_core}, device_id_type=MESH)

    def place(of_core, ch):
        return of_core if ch == 0 else num_chunks - 1 - of_core

    exchanged = ((q_hbm, q_buf), (do_hbm, do_buf), (st_hbm, st_buf))

    def ex_copies(h):
        for a, (src, dst) in enumerate(exchanged):
            for ch in range(2):
                mine = place(core, ch)
                yield (remote(src.at[(1 - core) * heads + h, ch], dst.at[h, mine], ex_send.at[h, a, ch], ex_recv.at[h, a, ch], chip, 1 - core),
                       remote(src.at[(1 - core) * heads + h, ch], dst.at[h, place(1 - core, ch)], ex_send.at[h, a, ch], ex_recv.at[h, a, ch], chip, 1 - core),
                       pltpu.make_async_copy(src.at[core * heads + h, ch], dst.at[h, mine], ex_local.at[h, a, ch]))

    def own_copies(h):
        for ch in range(2):
            mine = place(core, ch)
            yield (remote(kv_hbm.at[(1 - core) * heads + h, ch], kv_buf.at[0, h, mine], own_send.at[h, ch], own_kv_recv.at[h, ch], chip, 1 - core),
                   remote(kv_hbm.at[(1 - core) * heads + h, ch], kv_buf.at[0, h, place(1 - core, ch)], own_send.at[h, ch], own_kv_recv.at[h, ch], chip, 1 - core),
                   pltpu.make_async_copy(kv_hbm.at[core * heads + h, ch], kv_buf.at[0, h, mine], own_local.at[h, ch]))

    def nb_out(h, to_core, ch, way):
        return remote(kv_hbm.at[to_core * heads + h, ch], kv_buf.at[3 if way == 0 else 1, h, place(core, ch)],
                      nb_send.at[h, to_core, ch, way], nb_recv.at[h, place(core, ch), way], right if way == 0 else left, to_core)

    def second_sent(way):
        return chip >= 2 if way == 0 else chip >= 1

    def nb_each(h, fn):
        for way in range(2):
            for to_core in range(CORES):
                fn(nb_out(h, to_core, 0, way))

            @pl.when(second_sent(way))
            def _():
                for to_core in range(CORES):
                    fn(nb_out(h, to_core, 1, way))

    def nb_wait(h, way):
        slot = 3 if way == 0 else 1

        def wait(idx):
            remote(kv_hbm.at[0, 0], kv_buf.at[slot, h, idx], nb_send.at[h, 0, 0, way], nb_recv.at[h, idx, way], left, core).wait_recv()

        wait(0)
        wait(1)

        @pl.when(left >= 2 if way == 0 else right >= 1)
        def _():
            wait(2)
            wait(3)

    def relay(h, second, kind):
        src_slot, to_chip = (3, right) if kind == 0 else (1, left)
        pair = pl.ds(2 * second, 2)
        return remote(kv_buf.at[src_slot, h, pair, kind], kv_buf.at[2, h, pair, kind], rl_send.at[h, second, kind], op_recv.at[h, second, kind], to_chip, core)

    def relay_each(h, fn):
        for kind in range(2):
            fn(relay(h, 0, kind))

            @pl.when(right < left if kind == 0 else left < right)
            def _():
                fn(relay(h, 1, kind))

    def part_out(h, off, idx):
        to_chip = right if off == 1 else left
        home_core = idx if idx < 2 else num_chunks - 1 - idx
        return remote(send_buf.at[h, off - 1, idx], part.at[2 if off == 1 else 0, core * heads + h, idx // 2],
                      pt_send.at[h, off // 2, idx], pt_recv.at[1 if off == 1 else 0, core * heads + h, idx // 2], to_chip, home_core)

    def transit_out(h, second, kind):
        pair = pl.ds(2 * second, 2)
        return remote(send_buf.at[h, 1, pair, kind], transit.at[h, kind, pair], tr_send.at[h, second, kind], tr_recv.at[h, second, kind],
                      right if kind == 0 else left, core)

    def forward_out(h, idx, kind):
        home_core = idx if idx < 2 else num_chunks - 1 - idx
        return remote(transit.at[h, kind, idx], part.at[1, core * heads + h, idx // 2, kind],
                      fw_send.at[h, idx, kind], fw_recv.at[core * heads + h, idx // 2, kind], right if kind == 0 else left, home_core)

    def forward_each(h, fn):
        for kind in range(2):
            fn(h, 0, kind)

            @pl.when(left < right if kind == 0 else right < left)
            def _():
                fn(h, 1, kind)

    def start_forward(h, second, kind):
        transit_out(h, second, kind).wait_recv()
        for idx in (2 * second, 2 * second + 1):
            forward_out(h, idx, kind).start()

    def end_forward(h, second, kind):
        for idx in (2 * second, 2 * second + 1):
            forward_out(h, idx, kind).wait_send()

    def own_out(h, ch):
        return remote(own_acc.at[h, place(1 - core, ch)], own_recv.at[h, ch], oa_send.at[h, ch], oa_recv.at[h, ch], chip, 1 - core)

    def dq_copies(h):
        for ch in range(2):
            yield (remote(q_buf.at[h, place(1 - core, ch)], dq_hbm.at[core * heads + h, ch], dq_send.at[h, ch], dq_recv.at[h, ch], chip, 1 - core),
                   remote(q_buf.at[h, place(1 - core, ch)], dq_hbm.at[(1 - core) * heads + h, ch], dq_send.at[h, ch], dq_recv.at[h, ch], chip, 1 - core),
                   pltpu.make_async_copy(q_buf.at[h, place(core, ch)], dq_hbm.at[core * heads + h, ch], dq_local.at[h, ch]))

    def dw_out_to(step):
        peer = (me + step) % (num_chips * CORES)
        return remote(dw_acc, dw_all.at[me], dw_send.at[step], dw_recv.at[me], peer // CORES, peer % CORES)

    def block(h, off, kc, qb, masked, slot=0):
        k_blk, v_blk = kv_buf[off, h, kc, 0], kv_buf[off, h, kc, 1]
        if masked:
            key_pos = lax.broadcasted_iota(jnp.int32, (chunk_len, chunk_len), 0)
            query_pos = lax.broadcasted_iota(jnp.int32, (chunk_len, chunk_len), 1)
            visible = key_pos <= query_pos
        for g in range(per_kv):
            cols = pl.ds(g * chunk_len, chunk_len)
            logits = dot(k_blk, qt_now[qb, :, cols]) * (SM_SCALE * LOG2E) - st_buf[h, qb, 0, g:g + 1, :]
            if masked:
                logits = jnp.where(visible, logits, -jnp.inf)
            prob = jnp.exp2(logits)
            dprob = dot(v_blk, dot_now[qb, :, cols])
            p_now[slot, :, cols] = prob.astype(jnp.bfloat16)
            ds_now[slot, :, cols] = (prob * (dprob - st_buf[h, qb, 1, g:g + 1, :])).astype(jnp.bfloat16)
        acc[kc, 1] += dot(p_now[slot], do_buf[h, qb])
        acc[kc, 0] += dot(ds_now[slot], q_now[qb])
        dqt_now[qb] += dot(kt_now[...], ds_now[slot])

    def source_block(h, off):
        src = (chip + off) % num_chips
        own = off == 0
        early = src < chip
        acc[...] = jnp.zeros_like(acc)

        @pl.loop(0, jnp.where(early, num_chunks // 2, num_chunks))
        def _(kc):
            kt_now[...] = kv_buf[off, h, kc, 0].T

            @pl.when(own)
            def _():
                block(h, off, kc, kc, True)

                @pl.loop(kc + 1, num_chunks)
                def _(qb):
                    block(h, off, kc, qb, False)

            @pl.when(jnp.logical_not(own))
            def _():
                @pl.loop(jnp.where(early, 0, num_chunks // 4), num_chunks // 2)
                def _(pair):
                    block(h, off, kc, 2 * pair, False)
                    block(h, off, kc, 2 * pair + 1, False, 1)

    def home(head, h, own):
        for ch in range(2):
            mine = place(core, ch)
            total[...] = own_acc[h, mine] if own else own_recv[h, ch]

            def add(slot):
                total[...] += part[slot, head, ch].astype(jnp.float32)

            def take_side(way):
                remote(send_buf.at[0, 0, 0], part.at[2 * way, head, ch], pt_send.at[0, 0, 0], pt_recv.at[way, head, ch], left, core).wait_recv()
                add(2 * way)

            def take_far():
                for kind in range(2):
                    remote(transit.at[0, 0, 0], part.at[1, head, ch, kind], fw_send.at[0, 0, 0], fw_recv.at[head, ch, kind], left, core).wait_recv()
                add(1)

            if ch == 0:
                take_side(0)
                take_side(1)
                take_far()
            else:
                @pl.when(right < chip)
                def _():
                    take_side(0)

                @pl.when(left < chip)
                def _():
                    take_side(1)

                @pl.when(far < chip)
                def _():
                    take_far()

            raw = k_raw[head, ch].astype(jnp.float32)
            grad_raw, terms = norm_rope_pull(raw, wk[...], cos_k[ch], sin_k[ch], total[0] * SM_SCALE)
            dkv_out[head, 0, ch] = grad_raw.astype(jnp.bfloat16)
            dkv_out[head, 1, ch] = total[1].astype(jnp.bfloat16)
            dw_acc[1] += terms
        out_copy(head).start()

    def home_head(h):
        for ch in range(2):
            own_out(h, ch).wait_recv()
            own_out(h, ch).wait_send()
        home((1 - core) * heads + h, h, False)
        home(core * heads + h, h, True)

    def compute_head(h):
        for copies in (own_copies(h), ex_copies(h)):
            for out, arriving, local in copies:
                out.wait_send()
                arriving.wait_recv()
                local.wait()
        dqt_now[...] = jnp.zeros_like(dqt_now)

        @pl.loop(0, num_chunks)
        def _(qb):
            for g in range(per_kv):
                rows = pl.ds(g * chunk_len, chunk_len)
                raw_bf = q_buf[h, qb, rows, :].T
                raw_now[qb, :, rows] = raw_bf
                raw = raw_bf.astype(jnp.float32)
                normed = raw * inverse_rms_t(raw) * wq[...]
                query = (normed * cos_q[qb] + swap_rows(normed) * sin_q[qb]).astype(jnp.bfloat16)
                qt_now[qb, :, rows] = query
                q_now[qb, rows, :] = query.T
            dot_now[qb] = do_buf[h, qb].T

        last = h == heads - 1

        @pl.loop(0, num_chips)
        def _(j):
            orders = [sum(off * 4 ** i for i, off in enumerate(order)) for order in ((0, 3, 1, 2), (0, 1, 3, 2), (3, 1, 0, 2), (2, 1, 3, 0))]
            order = jnp.where(h == 0, orders[0], jnp.where(last, orders[3], jnp.where(h == 1, orders[1], orders[2])))
            off = order // jnp.where(j == 0, 1, jnp.where(j == 1, 4, jnp.where(j == 2, 16, 64))) % 4

            @pl.when(off == 2)
            def _():
                for kind in range(2):
                    relay(h, 0, kind).wait_recv()

                @pl.when(chip < far)
                def _():
                    for kind in range(2):
                        relay(h, 1, kind).wait_recv()

            source_block(h, off)
            src = (chip + off) % num_chips

            @pl.when(off == 0)
            def _():
                own_acc[h] = acc[...]
                for ch in range(2):
                    own_out(h, ch).start()

            @pl.when(off != 0)
            def _():
                send_buf[h, off - 1, 0:2] = acc[0:2].astype(jnp.bfloat16)

                @pl.when(chip < src)
                def _():
                    send_buf[h, off - 1, 2:4] = acc[2:4].astype(jnp.bfloat16)

            for side in (1, 3):
                @pl.when(off == side)
                def _():
                    part_out(h, side, 0).start()
                    part_out(h, side, 1).start()

                    @pl.when(chip < src)
                    def _():
                        part_out(h, side, 2).start()
                        part_out(h, side, 3).start()

            @pl.when(off == 2)
            def _():
                for kind in range(2):
                    transit_out(h, 0, kind).start()

                @pl.when(chip < src)
                def _():
                    for kind in range(2):
                        transit_out(h, 1, kind).start()

            def pass_keys(of_head):
                nb_wait(of_head, 0)
                nb_wait(of_head, 1)
                relay_each(of_head, lambda copy: copy.start())

            @pl.when((h == 0) & (j == 0))
            def _():
                pass_keys(0)

            @pl.when((h + 1 < heads) & (j == jnp.where(h == 0, 2, 0)))
            def _():
                pass_keys(h + 1)

            @pl.when((h + 2 < heads) & (j == jnp.where(h == 0, 1, 0)))
            def _():
                nb_each(h + 2, lambda copy: copy.start())

            @pl.when((h > 0) & (j == jnp.where(last, 0, 2)))
            def _():
                forward_each(h - 1, start_forward)

            @pl.when(last & (j == 1))
            def _():
                forward_each(h, start_forward)

        @pl.loop(0, num_chunks)
        def _(qb):
            for g in range(per_kv):
                rows = pl.ds(g * chunk_len, chunk_len)
                grad = dqt_now[qb, :, rows] * SM_SCALE
                raw = raw_now[qb, :, rows].astype(jnp.float32)
                inv_rms = inverse_rms_t(raw)
                unit = raw * inv_rms
                grad_normed = grad * cos_q[qb] - swap_rows(grad) * sin_q[qb]
                dwq_acc[...] += grad_normed * unit
                grad_unit = grad_normed * wq[...]
                grad_raw = inv_rms * (grad_unit - unit * jnp.mean(grad_unit * unit, axis=0, keepdims=True))
                q_buf[h, qb, rows, :] = grad_raw.astype(jnp.bfloat16).T

        for out, _, local in dq_copies(h):
            out.start()
            local.start()

    barrier = pltpu.get_barrier_semaphore()
    for step in range(1, num_chips * CORES):
        pl.semaphore_signal(barrier, inc=1, device_id={'cp': (me + step) % (num_chips * CORES)}, device_id_type=MESH)
    pl.semaphore_wait(barrier, num_chips * CORES - 1)

    nb_each(0, lambda copy: copy.start())
    in_copy(0).start()

    @pl.loop(0, heads)
    def _(h):
        for out, _, local in own_copies(h):
            out.start()
            local.start()
        for out, _, local in ex_copies(h):
            out.start()
            local.start()

    nb_each(1, lambda copy: copy.start())
    in_copy(1).start()
    in_copy(2).start()
    wq[...] = jnp.broadcast_to(wq_row[...], (chunk_len, HEAD_DIM)).T
    in_copy(0).wait()
    dw_acc[...] = jnp.zeros_like(dw_acc)
    dwq_acc[...] = jnp.zeros_like(dwq_acc)

    @pl.loop(0, heads + 3)
    def _(h):
        @pl.when(h < heads)
        def _():
            compute_head(h)

        @pl.when(h == 3)
        def _():
            in_copy(1).wait()
            in_copy(2).wait()

        @pl.when(h >= 3)
        def _():
            home_head(h - 3)

    dw_acc[0] = dwq_acc[...].T.reshape(-1, 8, HEAD_DIM).sum(0)
    for step in range(1, num_chips * CORES):
        dw_out_to(step).start()
    dw_all[me] = dw_acc[...]

    @pl.loop(0, heads)
    def _(h):
        nb_each(h, lambda copy: copy.wait_send())
        relay_each(h, lambda copy: copy.wait_send())
        for off in (1, 3):
            part_out(h, off, 0).wait_send()
            part_out(h, off, 1).wait_send()

            @pl.when(chip < (chip + off) % num_chips)
            def _():
                part_out(h, off, 2).wait_send()
                part_out(h, off, 3).wait_send()
        for kind in range(2):
            transit_out(h, 0, kind).wait_send()

        @pl.when(chip < far)
        def _():
            for kind in range(2):
                transit_out(h, 1, kind).wait_send()
        forward_each(h, end_forward)
        for out, arriving, local in dq_copies(h):
            out.wait_send()
            arriving.wait_recv()
            local.wait()
        out_copy(h).wait()
        out_copy(heads + h).wait()

    for step in range(1, num_chips * CORES):
        peer = (me + step) % (num_chips * CORES)
        dw_out_to(step).wait_send()
        remote(dw_acc, dw_all.at[peer], dw_send.at[step], dw_recv.at[peer], chip, core).wait_recv()
    dw_out[...] = dw_all[...].sum(0).sum(1)


def prepare_kernel(q_ref, do_ref, out_ref, k_ref, v_ref, lse_ref, k_table, wk, q_out, do_out, st_out, kv_out, k_out):
    rows, num_heads = q_ref.shape[0], q_ref.shape[1]
    kv_heads = k_ref.shape[1]
    f32, bf16 = jnp.float32, jnp.bfloat16

    def by_head(arr):
        return jnp.swapaxes(arr, 0, 1)

    d_out = do_ref[...].astype(f32)
    q_out[:, 0] = by_head(q_ref[...].astype(f32)).astype(bf16).reshape(kv_heads, -1, rows, HEAD_DIM)
    do_out[:, 0] = by_head(d_out).astype(bf16).reshape(kv_heads, -1, rows, HEAD_DIM)
    delta = jnp.sum(d_out * out_ref[...].astype(f32), axis=-1)
    st_out[:, 0, 0] = (lse_ref[...] * LOG2E).reshape(kv_heads, -1, rows)
    st_out[:, 0, 1] = delta.T.reshape(kv_heads, -1, rows)
    raw = k_ref[...].astype(f32)
    normed = raw * inverse_rms(raw) * wk[...]
    key = normed * k_table[0, 0][:, None] + swap_halves(normed) * k_table[1, 0][:, None]
    kv_out[:, 0, 0] = by_head(key).astype(bf16)
    kv_out[:, 0, 1] = by_head(v_ref[...].astype(f32)).astype(bf16)
    k_out[:, 0] = by_head(raw).astype(bf16)


def prepare(q_raw, d_out, out_fwd, k_raw, v_proj, lse_t, k_tables, wk, rows=128):
    local_rows, num_heads, _ = q_raw.shape
    kv_heads = k_raw.shape[1]
    per_kv, chunk_len = num_heads // kv_heads, local_rows // 2
    parts = chunk_len // rows
    bf16 = jnp.bfloat16
    rows_q = pl.BlockSpec((rows, num_heads, HEAD_DIM), lambda i: (i, 0, 0))
    rows_k = pl.BlockSpec((rows, kv_heads, HEAD_DIM), lambda i: (i, 0, 0))
    table = pl.BlockSpec((2, 1, rows, HEAD_DIM), lambda i: (0, i // parts, i % parts, 0))
    heads_q = pl.BlockSpec((kv_heads, 1, per_kv, rows, HEAD_DIM), lambda i: (0, i // parts, 0, i % parts, 0))
    return pl.pallas_call(
        prepare_kernel,
        grid=(2 * parts,),
        in_specs=[rows_q, rows_q, rows_q, rows_k, rows_k, pl.BlockSpec((num_heads, rows), lambda i: (0, i)), table,
                  pl.BlockSpec((1, HEAD_DIM), lambda i: (0, 0))],
        out_specs=[heads_q, heads_q,
                   pl.BlockSpec((kv_heads, 1, 2, per_kv, rows), lambda i: (0, i // parts, 0, 0, i % parts)),
                   pl.BlockSpec((kv_heads, 1, 2, rows, HEAD_DIM), lambda i: (0, i // parts, 0, i % parts, 0)),
                   pl.BlockSpec((kv_heads, 1, rows, HEAD_DIM), lambda i: (0, i // parts, i % parts, 0))],
        out_shape=[jax.ShapeDtypeStruct((kv_heads, 2, per_kv, chunk_len, HEAD_DIM), bf16),
                   jax.ShapeDtypeStruct((kv_heads, 2, per_kv, chunk_len, HEAD_DIM), bf16),
                   jax.ShapeDtypeStruct((kv_heads, 2, 2, per_kv, chunk_len), jnp.float32),
                   jax.ShapeDtypeStruct((kv_heads, 2, 2, chunk_len, HEAD_DIM), bf16),
                   jax.ShapeDtypeStruct((kv_heads, 2, chunk_len, HEAD_DIM), bf16)],
        compiler_params=pltpu.CompilerParams(vmem_limit_bytes=63 * 2 ** 20),
        name='prepare',
    )(q_raw, d_out, out_fwd, k_raw, v_proj, lse_t, k_tables, wk)


def finish_kernel(dq_ref, dkv_ref, dq_out, dk_out, dv_out):
    for src, dst in ((dq_ref, dq_out), (dkv_ref.at[:, 0], dk_out), (dkv_ref.at[:, 1], dv_out)):
        by_head = src[:, 0].reshape(-1, src.shape[-2], HEAD_DIM).astype(jnp.float32)
        dst[...] = jnp.swapaxes(by_head, 0, 1).astype(jnp.bfloat16)


def finish(dq, dkv, rows=64):
    kv_heads, _, per_kv, chunk_len, _ = dq.shape
    parts = chunk_len // rows
    num_heads = kv_heads * per_kv
    heads_k = pl.BlockSpec((kv_heads, 2, 1, rows, HEAD_DIM), lambda i: (0, 0, i // parts, i % parts, 0))
    rows_k = pl.BlockSpec((rows, kv_heads, HEAD_DIM), lambda i: (i, 0, 0))
    out_k = jax.ShapeDtypeStruct((2 * chunk_len, kv_heads, HEAD_DIM), jnp.bfloat16)
    return pl.pallas_call(
        finish_kernel,
        grid=(2 * parts,),
        in_specs=[pl.BlockSpec((kv_heads, 1, per_kv, rows, HEAD_DIM), lambda i: (0, i // parts, 0, i % parts, 0)), heads_k],
        out_specs=[pl.BlockSpec((rows, num_heads, HEAD_DIM), lambda i: (i, 0, 0)), rows_k, rows_k],
        out_shape=[jax.ShapeDtypeStruct((2 * chunk_len, num_heads, HEAD_DIM), jnp.bfloat16), out_k, out_k],
        compiler_params=pltpu.CompilerParams(vmem_limit_bytes=63 * 2 ** 20),
        name='finish',
    )(dq, dkv)


def attn_grads(num_chips, q, d_out, stats, kv, k_raw, tables, k_tables, wq, wk):
    kv_heads, _, rows, _ = q.shape
    chunk_len = kv.shape[3]
    heads = kv_heads // CORES
    half = (2, chunk_len, HEAD_DIM)
    bf16, f32 = jnp.bfloat16, jnp.float32
    sem = pltpu.SemaphoreType.DMA
    any_spec, vmem = pl.BlockSpec(memory_space=pl.ANY), pl.BlockSpec(memory_space=pltpu.VMEM)
    return pl.pallas_call(
        functools.partial(attn_kernel, num_chips),
        in_specs=[any_spec] * 7 + [vmem] * 2,
        out_specs=[any_spec, any_spec, vmem],
        out_shape=[jax.ShapeDtypeStruct(q.shape, bf16), jax.ShapeDtypeStruct((kv_heads, 2) + k_raw.shape[1:], bf16),
                   jax.ShapeDtypeStruct((2, HEAD_DIM), f32)],
        scratch_shapes=[
            pltpu.VMEM(k_raw.shape, bf16),
            pltpu.VMEM(tables.shape, f32),
            pltpu.VMEM(k_tables.shape, f32),
            pltpu.VMEM((HEAD_DIM, chunk_len), f32),
            pltpu.VMEM((kv_heads, 2) + k_raw.shape[1:], bf16),
            pltpu.VMEM((heads, 4, rows, HEAD_DIM), bf16),
            pltpu.VMEM((heads, 4, rows, HEAD_DIM), bf16),
            pltpu.VMEM((heads, 4) + stats.shape[2:], f32),
            pltpu.VMEM((num_chips, heads, 4) + half, bf16),
            pltpu.VMEM((4, HEAD_DIM, rows), bf16),
            pltpu.VMEM((4, rows, HEAD_DIM), bf16),
            pltpu.VMEM((4, HEAD_DIM, rows), bf16),
            pltpu.VMEM((4, HEAD_DIM, rows), bf16),
            pltpu.VMEM((4, HEAD_DIM, rows), f32),
            pltpu.VMEM((HEAD_DIM, chunk_len), bf16),
            pltpu.VMEM((2, chunk_len, rows), bf16),
            pltpu.VMEM((2, chunk_len, rows), bf16),
            pltpu.VMEM((4,) + half, f32),
            pltpu.VMEM((heads, 4) + half, f32),
            pltpu.VMEM((heads, 2) + half, f32),
            pltpu.VMEM((heads, 3, 4) + half, bf16),
            pltpu.VMEM((heads, 2, 4, chunk_len, HEAD_DIM), bf16),
            pltpu.VMEM((3, kv_heads, 2) + half, bf16),
            pltpu.VMEM(half, f32),
            pltpu.VMEM((HEAD_DIM, chunk_len), f32),
            pltpu.VMEM((2, 8, HEAD_DIM), f32),
            pltpu.VMEM((num_chips * CORES, 2, 8, HEAD_DIM), f32),
            sem((heads, 3, 2)), sem((heads, 3, 2)), sem((heads, 3, 2)),
            sem((heads, 2)), sem((heads, 2)), sem((heads, 2)),
            sem((heads, CORES, 2, 2)), sem((heads, 4, 2)),
            sem((heads, 2, 2)), sem((heads, 2, 2)),
            sem((heads, 2, 4)), sem((2, kv_heads, 2)),
            sem((heads, 2, 2)), sem((heads, 2, 2)),
            sem((heads, 4, 2)), sem((kv_heads, 2, 2)),
            sem((heads, 2)), sem((heads, 2)),
            sem((heads, 2)), sem((heads, 2)), sem((heads, 2)),
            sem((num_chips * CORES,)), sem((num_chips * CORES,)),
            sem((3,)), sem((kv_heads,)),
        ],
        compiler_params=pltpu.CompilerParams(vmem_limit_bytes=63 * 2 ** 20, collective_id=0, has_side_effects=True),
        cost_estimate=pl.CostEstimate(flops=50_000_000_000, bytes_accessed=64_000_000, transcendentals=40_000_000),
        name='attn_grads',
    )(q, d_out, stats, kv, k_raw, tables, k_tables, wq, wk)


def solution(mesh):
    cp_size = mesh.shape['cp']
    num_chips = cp_size // CORES

    def local_grads(q_raw, k_raw, v_proj, out_fwd, lse_fwd, d_out, q_norm, k_norm):
        dev_rank = lax.axis_index('cp')
        chip = dev_rank // CORES
        local_rows, num_heads = q_raw.shape[0], q_raw.shape[1]
        chunk_len = local_rows // 2
        kv_heads = k_raw.shape[1]
        per_kv = num_heads // kv_heads

        num_chunks = 2 * cp_size
        offsets = jnp.arange(chunk_len)
        chip_chunks = jnp.stack([2 * chip, 2 * chip + 1, num_chunks - 2 - 2 * chip, num_chunks - 1 - 2 * chip])
        inv_freq = ROPE_THETA ** (-jnp.arange(0, HEAD_DIM, 2).astype(jnp.float32) / HEAD_DIM)
        angles = inv_freq[None, :, None] * (chip_chunks[:, None] * chunk_len + offsets).astype(jnp.float32)[:, None, :]
        cos_t, sin_t = jnp.cos(angles), jnp.sin(angles)
        tables = jnp.stack([jnp.concatenate([cos_t, cos_t], axis=1), jnp.concatenate([-sin_t, sin_t], axis=1)])
        dev_chunks = jnp.stack([dev_rank, num_chunks - 1 - dev_rank])
        k_tables = jnp.stack(rope_tables(dev_chunks[:, None] * chunk_len + offsets))

        q_h, do_h, stats, kv, k_h = prepare(q_raw, d_out, out_fwd, k_raw, v_proj, lse_fwd.T, k_tables, k_norm[None])
        stacked = (kv_heads, 2, per_kv * chunk_len, HEAD_DIM)
        dq, dkv, weights = attn_grads(num_chips, q_h.reshape(stacked), do_h.reshape(stacked), stats, kv, k_h,
                                      tables, k_tables, q_norm[None], k_norm[None])
        dq_raw, dk_raw, dv_home = finish(dq.reshape(q_h.shape), dkv)
        return dq_raw, dk_raw, dv_home, weights[0], weights[1]

    row_spec = P(('dp', 'cp'))
    in_specs = (row_spec, row_spec, row_spec, row_spec, row_spec, row_spec, P(), P())
    out_specs = (row_spec, row_spec, row_spec, P('dp'), P('dp'))
    return jax.shard_map(local_grads, mesh=mesh, in_specs=in_specs, out_specs=out_specs, check_vma=False)
```
